128 devices in a mesh: outer: 16 (over y, x), span: 8 (over z, core).
Axes of the slice: x: 4, y: 4, z: 4, core: 2. Of those that a mesh axis runs over, the one named last changes fastest.
Arguments:
- queries_in: bfloat16 [32, 4096, 16, 128], P('outer', 'span'), may hold values from -6 to 6
- keys_in: bfloat16 [32, 4096, 16, 128], P('outer', 'span'), may hold values from -6 to 6
- values_in: bfloat16 [32, 4096, 16, 128], P('outer', 'span'), may hold values from -6 to 6
- gate_rows: bfloat16 [32, 4096, 16, 128], P('outer', 'span'), may hold values from -6 to 6
- out_weight: bfloat16 [2048, 2048], P('outer'), may hold values from -0.125 to 0.125
Outputs:
- mixer_out: bfloat16 [32, 4096, 2048], P('outer', 'span')
The draws below stay inside these ranges and needn't reach their ends.
All inputs are finite; a program needn't handle non-finite values.
Results may differ from the reference program's by a relative error of at most 0.0023.
Values may be sent and summed in bfloat16 or wider, within the bound.
A program may use at most 256 MiB of HBM per device.

```python
import jax
import jax.numpy as jnp
from jax import lax

HEADS = 16
HEAD_SIZE = 128
BATCH = 32
TOKENS = 4096
WIDTH = 2048


def block_scale(own_key, dims, shards, low, largest):
    def one(position, parts):
        heights = jax.random.uniform(jax.random.fold_in(jax.random.fold_in(own_key, 6), position), (parts,), jnp.float32, low / len(shards), largest / len(shards))
        return jnp.repeat(jnp.exp(heights), dims[position] // parts).reshape((-1,) + (1,) * (len(dims) - position - 1))

    factor_of = one(*shards[0])
    for cut in shards[1:]:
        factor_of = factor_of * one(*cut)
    return factor_of


def scatter_about(own_key, dims, deviation, reach, shards=(), kind=jnp.bfloat16):
    entries = deviation * jax.random.normal(own_key, dims, jnp.float32)
    if shards:
        entries = entries * block_scale(own_key, dims, shards, -0.22, 0.18)
    return jnp.clip(entries, -reach, reach).astype(kind)


def setup_inputs(seed: int = 0) -> dict:
    streams_of = jax.random.split(jax.random.key(seed), 6)
    return {
        "queries_in": scatter_about(streams_of[0], (BATCH, TOKENS, HEADS, HEAD_SIZE), 1.0, 6.0, ((0, 16), (1, 8))),
        "keys_in": scatter_about(streams_of[1], (BATCH, TOKENS, HEADS, HEAD_SIZE), 1.0, 6.0, ((0, 16), (1, 8))),
        "values_in": scatter_about(streams_of[2], (BATCH, TOKENS, HEADS, HEAD_SIZE), 1.0, 6.0, ((0, 16), (1, 8))),
        "gate_rows": scatter_about(streams_of[3], (BATCH, TOKENS, HEADS, HEAD_SIZE), 1.0, 6.0, ((0, 16), (1, 8))),
        "out_weight": scatter_about(streams_of[4], (WIDTH, WIDTH), WIDTH ** -0.5, 0.125, ((0, 16),)),
    }


def feature_map(values):
    wide = values.astype(jnp.float32)
    return (jnp.where(wide > 0.0, wide + 1.0, jnp.exp(jnp.minimum(wide, 0.0)))).astype(jnp.bfloat16)


def close_heads(read, gate_rows, count):
    result = read * count ** 0.5
    result = result * jax.nn.sigmoid(gate_rows.astype(jnp.float32))
    return result.astype(jnp.bfloat16)


def ask_state(features, state, mass):
    small = lax.optimization_barrier(state.astype(jnp.bfloat16))
    top = jnp.einsum("bthd,bhde->bthe", features.astype(jnp.float32), small.astype(jnp.float32))
    bottom = jnp.einsum("bthd,bhd->bth", features.astype(jnp.float32), mass, precision=lax.Precision.HIGHEST)
    return top / (bottom + 1e-3)[..., None]


def reference(queries_in, keys_in, values_in, gate_rows, out_weight):
    query_feature, key_feature = lax.optimization_barrier((feature_map(queries_in), feature_map(keys_in)))
    state = jnp.einsum("bthd,bthe->bhde", key_feature.astype(jnp.float32), values_in.astype(jnp.float32)) / TOKENS
    mass = jnp.sum(key_feature.astype(jnp.float32), axis=1) / TOKENS
    mixed = close_heads(ask_state(query_feature, state, mass), gate_rows, TOKENS).reshape(BATCH, TOKENS, WIDTH)
    mixed = lax.optimization_barrier(mixed)
    mixer_out = jnp.einsum("btw,wv->btv", mixed.astype(jnp.float32), out_weight.astype(jnp.float32)).astype(jnp.bfloat16)
    return mixer_out
```

```python
import functools
import jax
import jax.numpy as jnp
from jax import lax
from jax.experimental import pallas as pl
from jax.experimental.pallas import tpu as pltpu
from jax.sharding import PartitionSpec as P

f32 = jnp.float32
bf16 = jnp.bfloat16
MESH = pl.DeviceIdType.MESH

SEQS = 2
T = 512
HEADS = 16
D = 128
WIDTH = HEADS * D
COUNT = 4096
PITCH = T + 4
TC = 64
HG = 4
PIECES = 4
ROWS = 32


def feature(x):
    return jnp.maximum(x, 0.0) + jnp.exp(jnp.minimum(x, 0.0))


def spread(src, dst, seq, fn):
    def step(i, carry):
        start = i * TC
        values = fn(src[seq, pl.ds(start, TC)].astype(f32))
        for t in range(TC):
            for half in range(2):
                dst[pl.ds(start + t + 8 * half * PITCH, 8, stride=PITCH), :] = values[
                    t, 8 * half : 8 * half + 8, :
                ]
        return carry

    lax.fori_loop(0, T // TC, step, 0)


def attention(
    q_in, k_in, v_in, g_in, w_in,
    mixed_out, w_out,
    q_nat, k_nat, v_nat, g_nat,
    fa, fb, factor, q_head, part, mass, mass_in,
    core_in, zs1, zr1, zs2, zr2, state, mixed, w_buf,
    load_sem, w_load_sem, out_sem,
    core_send, core_recv, z_send, z_recv, st_send, st_recv, mass_send, mass_recv,
    ws_sem, wr_sem, wp_sem, wo_sem,
):
    o = lax.axis_index("outer")
    s = lax.axis_index("span")
    core = lax.rem(s, 2)
    z = lax.div(s, 2)
    other = s + 1 - 2 * core
    first = s + 2 * (1 - 2 * lax.rem(z, 2))
    second = 2 * (3 - z) + core
    sa = 1 + 3 * core
    sb = 4 - 3 * core
    a = lax.rem(lax.div(o, sa), 4)
    b = lax.rem(lax.div(o, sb), 4)

    def shard(da, db):
        return lax.rem(a + da, 4) * sa + lax.rem(b + db, 4) * sb

    arrays = (k_in, v_in, q_in, g_in)
    natural = (k_nat, v_nat, q_nat, g_nat)
    step = T // PIECES

    def load(i, seq, piece):
        rows = pl.ds(piece * step, step)
        return pltpu.make_async_copy(
            arrays[i].at[seq, rows], natural[i].at[seq, rows], load_sem.at[i, seq, piece]
        )

    def start_load(i, seq):
        for piece in range(PIECES):
            load(i, seq, piece).start()

    def wait_load(i, seq):
        for piece in range(PIECES):
            load(i, seq, piece).wait()

    start_load(0, 0)
    start_load(1, 0)
    own_w = pltpu.make_async_copy(w_in, w_buf.at[o], w_load_sem)
    own_w.start()
    start_load(0, 1)
    start_load(1, 1)
    for seq in range(SEQS):
        start_load(2, seq)
        start_load(3, seq)

    barrier = pltpu.get_barrier_semaphore()
    for da, db in ((1, 0), (3, 0), (0, 1), (0, 3)):
        pl.semaphore_signal(barrier, inc=1, device_id=(shard(da, db), s), device_id_type=MESH)
    for d in range(1, 8):
        pl.semaphore_signal(barrier, inc=1, device_id=(o, lax.rem(s + d, 8)), device_id_type=MESH)
    pl.semaphore_wait(barrier, 11)

    KINDS = {"A+": (1, 0), "A-": (3, 0), "B+": (0, 1), "B-": (0, 3)}

    def w_copy(kind, da, db, h):
        ref = w_buf.at[shard(da, db), core, h]
        if kind == "P":
            return pltpu.make_async_remote_copy(
                src_ref=ref, dst_ref=ref, send_sem=ws_sem.at[4, da, db, h], recv_sem=wp_sem.at[da, db, h],
                device_id=(o, other), device_id_type=MESH,
            )
        ka, kb = KINDS[kind]
        return pltpu.make_async_remote_copy(
            src_ref=ref,
            dst_ref=ref,
            send_sem=ws_sem.at[list(KINDS).index(kind), da, db, h],
            recv_sem=wr_sem.at[(da - ka) % 4, (db - kb) % 4, h],
            device_id=(shard(ka, kb), s),
            device_id_type=MESH,
        )

    def arrival(ref, sem):
        pltpu.make_async_remote_copy(
            src_ref=ref, dst_ref=ref, send_sem=ws_sem.at[0, 0, 0, 0], recv_sem=sem,
            device_id=(o, other), device_id_type=MESH,
        ).wait_recv()

    sent = []

    def w_send(kind, da, db, h):
        w_copy(kind, da, db, h).start()
        sent.append((kind, da, db, h))

    def w_arrive(da, db, h):
        arrival(w_buf.at[shard(da, db), core, h], wr_sem.at[da, db, h])
        if db == 0:
            if da == 3 and h == 0:
                w_send("A+", da, db, h)
            if da == 1 and h == 1:
                w_send("A-", da, db, h)
            w_send("B+", da, db, h)
            w_send("B-", da, db, h)
        elif db == 3 and h == 0:
            w_send("B+", da, db, h)
        elif db == 1 and h == 1:
            w_send("B-", da, db, h)
        w_send("P", da, db, h)
        w_store(shard(da, db), core, h, da, db, 0).start()

    def w_store(row, c, h, da, db, which):
        return pltpu.make_async_copy(
            w_buf.at[row, c, h], w_out.at[row, c, h], wo_sem.at[which, da, db, h]
        )

    def w_from_partner(da, db, h):
        row = shard(db, da)
        arrival(w_buf.at[row, 1 - core, h], wp_sem.at[da, db, h])
        w_store(row, 1 - core, h, da, db, 1).start()

    groups = []
    for da in (0, 3, 1, 2):
        if da == 0:
            groups.append([(3, 0, 0), (1, 0, 1), (0, 3, 0), (0, 1, 1)])
            groups.append([(3, 0, 1), (1, 0, 0), (0, 3, 1), (0, 1, 0)])
            groups.append([(2, 0, 0), (2, 0, 1), (0, 2, 0), (0, 2, 1)])
        else:
            groups.append([(da, 3, 0), (da, 1, 1)])
            groups.append([(da, 3, 1), (da, 1, 0)])
            groups.append([(da, 2, 0), (da, 2, 1)])

    def service(i):
        for chunk in groups[i]:
            w_arrive(*chunk)

    own_w.wait()
    for kinds, h in ((("A+", "B+"), 0), (("A-", "B-"), 1), (("A+", "B+"), 1), (("A-", "B-"), 0)):
        for kind in kinds:
            w_send(kind, 0, 0, h)
    for c in range(2):
        for h in range(2):
            w_store(o, c, h, 0, 0, c).start()

    mine = core * 8
    theirs = 8 - mine

    def heads(seq, base):
        def group(i, carry):
            for j in range(HG):
                h = base + i * HG + j
                key = fa[pl.ds(h * PITCH, T), :].astype(bf16)
                value = fb[pl.ds(h * PITCH, T), :].astype(bf16)
                part[seq * HEADS + h] = lax.dot_general(
                    key, value, (((0,), (0,)), ((), ())), preferred_element_type=f32
                )
                m = jnp.sum(key.astype(f32).reshape(T // 8, 8, D), axis=0)
                mass[pl.ds(seq * HEADS + h, 1), :] = jnp.sum(m, axis=0, keepdims=True)
            return carry

        lax.fori_loop(0, 8 // HG, group, 0)

    def core_copy(seq):
        return pltpu.make_async_remote_copy(
            src_ref=part.at[pl.ds(seq * HEADS + theirs, 8)], dst_ref=core_in.at[seq],
            send_sem=core_send.at[seq], recv_sem=core_recv.at[seq],
            device_id=(o, other), device_id_type=MESH,
        )

    def z_copy(seq, stage, half):
        peer = (first, second)[(stage + half) % 2]
        src, dst = ((zs1, zr1), (zs2, zr2))[stage]
        rows = pl.ds(4 * half, 4)
        return pltpu.make_async_remote_copy(
            src_ref=src.at[seq, rows], dst_ref=dst.at[seq, rows],
            send_sem=z_send.at[seq, stage, half], recv_sem=z_recv.at[seq, stage, half],
            device_id=(o, peer), device_id_type=MESH,
        )

    def state_copy(seq):
        rows = pl.ds(seq * HEADS + mine, 8)
        return pltpu.make_async_remote_copy(
            src_ref=state.at[rows], dst_ref=state.at[rows],
            send_sem=st_send.at[seq], recv_sem=st_recv.at[seq],
            device_id=(o, other), device_id_type=MESH,
        )

    def mass_copy(seq, d):
        return pltpu.make_async_remote_copy(
            src_ref=mass.at[pl.ds(seq * HEADS, HEADS)], dst_ref=mass_in.at[seq, d],
            send_sem=mass_send.at[seq, d], recv_sem=mass_recv.at[seq, d],
            device_id=(o, lax.rem(s + d, 8)), device_id_type=MESH,
        )

    def reduce(seq, stage):
        if stage == 0:
            core_copy(seq).wait_recv()
            extra, dst, at = core_in, zs1, 0
        elif stage == 1:
            extra, dst, at = zr1, zs2, 0
        else:
            extra, dst, at = zr2, state, seq * HEADS + mine
        if stage:
            z_copy(seq, stage - 1, 0).wait_recv()
            z_copy(seq, stage - 1, 1).wait_recv()

        def one(i, carry):
            for j in range(4):
                h = i * 4 + j
                total = part[seq * HEADS + mine + h] + extra[seq, h].astype(f32)
                if stage < 2:
                    part[seq * HEADS + mine + h] = total
                    dst[seq, h] = total.astype(bf16)
                else:
                    dst[at + h] = total.astype(bf16)
            return carry

        lax.fori_loop(0, 2, one, 0)
        if stage < 2:
            z_copy(seq, stage, 0).start()
            z_copy(seq, stage, 1).start()
        else:
            state_copy(seq).start()

    def local_state(seq):
        heads(seq, theirs)
        core_copy(seq).start()
        heads(seq, mine)
        for d in range(1, 8):
            mass_copy(seq, d).start()

    def take_mass(seq):
        for d in range(1, 8):
            mass_copy(seq, d).wait()
        rows = pl.ds(seq * HEADS, HEADS)
        total = mass[rows, :]
        for d in range(1, 8):
            total = total + mass_in[seq, d]
        mass[rows, :] = total

    def factors(seq):
        def group(i, carry):
            for j in range(HG):
                h = i * HG + j
                rows = pl.ds(h * PITCH, T)
                query = fa[rows, :].astype(bf16)
                q_head[seq * HEADS + h] = query
                m = mass[pl.ds(seq * HEADS + h, 1), :]
                bottom = jnp.sum(query.astype(f32) * m, axis=1, keepdims=True) + 0.001 * COUNT
                factor[seq, rows, :] = COUNT**0.5 / (bottom * factor[seq, rows, :])
            return carry

        lax.fori_loop(0, HEADS // HG, group, 0)

    def read(seq):
        state_copy(seq).wait_recv()

        def group(i, carry):
            for j in range(HG):
                h = i * HG + j
                top = jnp.dot(q_head[seq * HEADS + h], state[seq * HEADS + h], preferred_element_type=f32)
                columns = pl.ds(pl.multiple_of(h * D, D), D)
                mixed[seq, :, columns] = (top * factor[seq, pl.ds(h * PITCH, T), :]).astype(bf16)
            return carry

        lax.fori_loop(0, HEADS // HG, group, 0)
        pltpu.make_async_copy(mixed.at[seq], mixed_out.at[seq], out_sem.at[seq]).start()

    gate = lambda x: 1.0 + jnp.exp(-x)
    wait_load(0, 0)
    wait_load(1, 0)
    spread(k_nat, fa, 0, feature)
    spread(v_nat, fb, 0, lambda x: x)
    local_state(0)
    wait_load(0, 1)
    wait_load(1, 1)
    spread(k_nat, fa, 1, feature)
    spread(v_nat, fb, 1, lambda x: x)
    reduce(0, 0)
    local_state(1)
    service(0)
    wait_load(2, 0)
    wait_load(3, 0)
    spread(q_nat, fa, 0, feature)
    reduce(1, 0)
    spread(g_nat, factor.at[0], 0, gate)
    service(1)
    reduce(0, 1)
    take_mass(0)
    factors(0)
    reduce(1, 1)
    service(2)
    wait_load(2, 1)
    wait_load(3, 1)
    spread(q_nat, fa, 1, feature)
    spread(g_nat, factor.at[1], 1, gate)
    reduce(0, 2)
    take_mass(1)
    factors(1)
    reduce(1, 2)
    service(3)
    service(4)
    read(0)
    service(5)
    service(6)
    read(1)
    for i in range(7, len(groups)):
        service(i)
    for group in groups:
        for chunk in group:
            w_from_partner(*chunk)

    for item in sent:
        w_copy(*item).wait_send()
    for group in groups:
        for da, db, h in group:
            w_store(shard(da, db), core, h, da, db, 0).wait()
            w_store(shard(db, da), 1 - core, h, da, db, 1).wait()
    for c in range(2):
        for h in range(2):
            w_store(o, c, h, 0, 0, c).wait()
    for seq in range(SEQS):
        core_copy(seq).wait_send()
        state_copy(seq).wait_send()
        for stage in range(2):
            for half in range(2):
                z_copy(seq, stage, half).wait_send()
        pltpu.make_async_copy(mixed.at[seq], mixed_out.at[seq], out_sem.at[seq]).wait()


def body(queries_in, keys_in, values_in, gate_rows, out_weight):
    any_space = pl.BlockSpec(memory_space=pl.ANY)
    natural = pltpu.VMEM((SEQS, T, HEADS, D), bf16)
    wide = pltpu.VMEM((HEADS * PITCH, D), f32)
    exchange = pltpu.VMEM((SEQS, 8, D, D), bf16)
    dma = pltpu.SemaphoreType.DMA
    mixed, weight = pl.pallas_call(
        attention,
        out_shape=(
            jax.ShapeDtypeStruct((SEQS, T, WIDTH), bf16),
            jax.ShapeDtypeStruct((16, 2, 2, ROWS, WIDTH), bf16),
        ),
        in_specs=[any_space] * 5,
        out_specs=(any_space, any_space),
        scratch_shapes=[
            natural, natural, natural, natural,
            wide, wide, pltpu.VMEM((SEQS, HEADS * PITCH, D), f32),
            pltpu.VMEM((SEQS * HEADS, T, D), bf16),
            pltpu.VMEM((SEQS * HEADS, D, D), f32),
            pltpu.VMEM((SEQS * HEADS, D), f32),
            pltpu.VMEM((SEQS, 8, HEADS, D), f32),
            pltpu.VMEM((SEQS, 8, D, D), f32),
            exchange, exchange, exchange, exchange,
            pltpu.VMEM((SEQS * HEADS, D, D), bf16),
            pltpu.VMEM((SEQS, T, WIDTH), bf16),
            pltpu.VMEM((16, 2, 2, ROWS, WIDTH), bf16),
            dma((4, SEQS, PIECES)), dma, dma((SEQS,)),
            dma((SEQS,)), dma((SEQS,)), dma((SEQS, 2, 2)), dma((SEQS, 2, 2)),
            dma((SEQS,)), dma((SEQS,)), dma((SEQS, 8)), dma((SEQS, 8)),
            dma((5, 4, 4, 2)), dma((4, 4, 2)), dma((4, 4, 2)), dma((2, 4, 4, 2)),
        ],
        compiler_params=pltpu.CompilerParams(
            collective_id=0, has_side_effects=True, vmem_limit_bytes=63 * 1024 * 1024
        ),
        name="attention",
    )(queries_in, keys_in, values_in, gate_rows, out_weight.reshape(2, 2, ROWS, WIDTH))
    weight = weight.reshape(WIDTH, WIDTH)
    return jnp.einsum("btw,wv->btv", mixed, weight, preferred_element_type=f32).astype(bf16)


def solution(mesh):
    rows = P("outer", "span", None, None)
    return jax.shard_map(
        body, mesh=mesh, in_specs=(rows, rows, rows, rows, P("outer", None)),
        out_specs=P("outer", "span", None), check_vma=False,
    )
```

```python
import functools
import jax
import jax.numpy as jnp
from jax import lax
from jax.experimental import pallas as pl
from jax.experimental.pallas import tpu as pltpu
from jax.sharding import PartitionSpec as P

f32 = jnp.float32
bf16 = jnp.bfloat16
MESH = pl.DeviceIdType.MESH

SEQS = 2
T = 512
HEADS = 16
D = 128
WIDTH = HEADS * D
COUNT = 4096
PITCH = T + 4
TC = 64
HG = 4
PIECES = 4
ROWS = 32
CHUNKS = 4
CROWS = 4 * D

ORDER = (
    (3, 0, 0), (1, 0, 1), (0, 3, 0), (0, 1, 1), (3, 0, 1), (1, 0, 0), (0, 3, 1), (0, 1, 0),
    (2, 0, 0), (2, 0, 1), (3, 3, 0), (3, 1, 0), (1, 1, 1), (1, 3, 1), (0, 2, 0), (0, 2, 1),
    (3, 1, 1), (3, 3, 1), (1, 3, 0), (1, 1, 0), (2, 3, 0), (2, 1, 0), (2, 1, 1), (2, 3, 1),
    (3, 2, 0), (3, 2, 1), (1, 2, 0), (1, 2, 1), (2, 2, 0), (2, 2, 1),
)
ARRIVE = (
    4.7, 4.7, 4.7, 4.7, 7.5, 7.5, 7.5, 7.5, 10.3, 10.3, 10.3, 10.3, 11.7, 11.7, 13.1, 13.1,
    14.6, 14.6, 16.0, 16.0, 17.4, 17.4, 18.8, 18.8, 20.2, 21.6, 21.6, 21.6, 23.0, 23.0,
)
GROUPS = (
    ((0, 0), (3, 0), (1, 0), (0, 3), (0, 1), (2, 0), (0, 2), (3, 3)),
    ((3, 1), (1, 3), (1, 1), (2, 3), (3, 2), (2, 1), (1, 2), (2, 2)),
)


def make_plan():
    begin, weights_at = 2.0, 3.0
    units = []
    for seq in range(SEQS):
        for part in range(2):
            units.append((("key", seq, part), 0.5, ()))
        units.append((("value", seq), 0.35, ()))
        for group in range(2):
            for side in range(2):
                units.append((("heads", seq, group, side), 0.3, ()))
        units.append((("mass", seq), 0.05, ()))
    for seq in range(SEQS):
        for part in range(2):
            units.append((("query", seq, part), 0.5, ()))
        for part in range(2):
            units.append((("gate", seq, part), 0.4, ()))
        units.append((("take", seq), 0.15, ()))
        for part in range(4):
            units.append((("factor", seq, part), 0.35, ()))
    for seq in range(SEQS):
        for group in range(2):
            units.append((("last", 2 * seq + group), 0.02, (("sum", 4, 2 * seq + group),)))
        for part in range(4):
            units.append((("read", seq, part), 0.3, ()))
        for part in range(4):
            units.append((("project", 0, seq, part), 0.6, (("weight", 17),)))
    for seq in range(SEQS):
        for part in range(4):
            units.append((("project", 1, seq, part), 0.6, (("weight", 29),)))

    ready = {("weight", i): weights_at + at for i, at in enumerate(ARRIVE)}
    wire = (1.4, 0.7, 0.4, 0.7)
    plan, done, clock, at = [], set(), begin, 0
    while at < len(units) or ready:
        due = [e for e in ready if ready[e] <= clock]
        token = None
        if due:
            token = min(due, key=lambda e: (ready[e], e))
        elif at < len(units) and all(n in done for n in units[at][2]):
            token, cost, _ = units[at]
            at += 1
            clock += cost
            if token[0] == "heads" and token[3] == 0:
                ready["sum", 0, 2 * token[1] + token[2]] = clock + 1.6
        else:
            token = min(ready, key=lambda e: (ready[e], e))
            clock = ready[token]
        if token in ready:
            del ready[token]
            clock += 0.05 if token[0] == "weight" else (0.25, 0.15, 0.1, 0.02, 0.02)[token[1]]
            if token[0] == "sum" and token[1] < 4:
                ready["sum", token[1] + 1, token[2]] = clock + wire[token[1]] + 2.2
        done.add(token)
        plan.append(token)
    return plan


def feature(x):
    return jnp.maximum(x, 0.0) + jnp.exp(jnp.minimum(x, 0.0))


def spread(src, dst, seq, fn, low, high):
    def step(i, carry):
        start = i * TC
        values = fn(src[seq, pl.ds(start, TC)].astype(f32))
        for t in range(TC):
            for half in range(2):
                dst[pl.ds(start + t + 8 * half * PITCH, 8, stride=PITCH), :] = values[
                    t, 8 * half : 8 * half + 8, :
                ]
        return carry

    lax.fori_loop(low, high, step, 0)


def attention(
    q_in, k_in, v_in, g_in, w_in,
    out,
    q_nat, k_nat, v_nat, g_nat,
    fa, fb, factor, q_head, part, mass, mass_in,
    core_in, z1, z2, state, staged, w_buf,
    load_sem, w_load_sem, out_sem,
    core_send, core_recv, z_send, z_recv, st_send, st_recv, mass_send, mass_recv,
    ws_sem, wr_sem, wp_sem,
):
    o = lax.axis_index("outer")
    s = lax.axis_index("span")
    core = lax.rem(s, 2)
    z = lax.div(s, 2)
    other = s + 1 - 2 * core
    first = s + 2 * (1 - 2 * lax.rem(z, 2))
    second = 2 * (3 - z) + core
    upper = lax.div(z, 2)
    gray = lax.rem(z + upper, 2)
    sa = 1 + 3 * core
    sb = 4 - 3 * core
    a = lax.rem(lax.div(o, sa), 4)
    b = lax.rem(lax.div(o, sb), 4)

    def shard(da, db):
        return lax.rem(a + da, 4) * sa + lax.rem(b + db, 4) * sb

    arrays = (k_in, v_in, q_in, g_in)
    natural = (k_nat, v_nat, q_nat, g_nat)
    step = T // PIECES

    def load(i, seq, piece):
        rows = pl.ds(piece * step, step)
        return pltpu.make_async_copy(
            arrays[i].at[seq, rows], natural[i].at[seq, rows], load_sem.at[i, seq, piece]
        )

    own_w = pltpu.make_async_copy(w_in, w_buf.at[o], w_load_sem)
    own_w.start()
    for pair in ((0, 1), (2, 3)):
        for seq in range(SEQS):
            for i in pair:
                for piece in range(PIECES):
                    load(i, seq, piece).start()

    barrier = pltpu.get_barrier_semaphore()
    for da, db in ((1, 0), (3, 0), (0, 1), (0, 3)):
        pl.semaphore_signal(barrier, inc=1, device_id=(shard(da, db), s), device_id_type=MESH)
    for d in range(1, 8):
        pl.semaphore_signal(barrier, inc=1, device_id=(o, lax.rem(s + d, 8)), device_id_type=MESH)
    own_w.wait()
    pl.semaphore_wait(barrier, 11)

    kinds = {"A+": (1, 0), "A-": (3, 0), "B+": (0, 1), "B-": (0, 3)}
    sent = []

    def w_copy(kind, da, db, h):
        ref = w_buf.at[shard(da, db), core, h]
        if kind == "P":
            return pltpu.make_async_remote_copy(
                src_ref=ref, dst_ref=ref, send_sem=ws_sem.at[4, da, db, h], recv_sem=wp_sem.at[da, db, h],
                device_id=(o, other), device_id_type=MESH,
            )
        ka, kb = kinds[kind]
        return pltpu.make_async_remote_copy(
            src_ref=ref,
            dst_ref=ref,
            send_sem=ws_sem.at[list(kinds).index(kind), da, db, h],
            recv_sem=wr_sem.at[(da - ka) % 4, (db - kb) % 4, h],
            device_id=(shard(ka, kb), s),
            device_id_type=MESH,
        )

    def w_send(kind, da, db, h):
        w_copy(kind, da, db, h).start()
        sent.append((kind, da, db, h))

    def arrival(ref, sem):
        pltpu.make_async_remote_copy(
            src_ref=ref, dst_ref=ref, send_sem=ws_sem.at[0, 0, 0, 0], recv_sem=sem,
            device_id=(o, other), device_id_type=MESH,
        ).wait_recv()

    def w_arrive(da, db, h):
        arrival(w_buf.at[shard(da, db), core, h], wr_sem.at[da, db, h])
        if db == 0:
            if da == 3 and h == 0:
                w_send("A+", da, db, h)
            if da == 1 and h == 1:
                w_send("A-", da, db, h)
            w_send("B+", da, db, h)
            w_send("B-", da, db, h)
        elif db == 3 and h == 0:
            w_send("B+", da, db, h)
        elif db == 1 and h == 1:
            w_send("B-", da, db, h)
        w_send("P", da, db, h)

    for names, h in ((("A+", "B+"), 0), (("A-", "B-"), 1), (("A+", "B+"), 1), (("A-", "B-"), 0)):
        for name in names:
            w_send(name, 0, 0, h)

    mine = core * 8
    theirs = 8 - mine

    def heads(seq, base):
        for j in range(HG):
            h = base + j
            key = fa[pl.ds(h * PITCH, T), :].astype(bf16)
            value = fb[pl.ds(h * PITCH, T), :].astype(bf16)
            part[pl.ds((seq * HEADS + h) * D, D), :] = lax.dot_general(
                key, value, (((0,), (0,)), ((), ())), preferred_element_type=f32
            )
            m = jnp.sum(key.astype(f32).reshape(T // 8, 8, D), axis=0)
            mass[pl.ds(seq * HEADS + h, 1), :] = jnp.sum(m, axis=0, keepdims=True)

    def base_row(c, side):
        return ((c // 2) * HEADS + (theirs if side else mine) + 4 * (c % 2)) * D

    def core_copy(c):
        return pltpu.make_async_remote_copy(
            src_ref=part.at[pl.ds(base_row(c, 1), CROWS)], dst_ref=core_in.at[c],
            send_sem=core_send.at[c], recv_sem=core_recv.at[c],
            device_id=(o, other), device_id_type=MESH,
        )

    half_rows, quarter, eighth = CROWS // 2, CROWS // 4, CROWS // 8
    bits = ((gray, upper), (upper, gray))
    peers = ((first, second), (second, first))

    def kept(side, depth):
        at = side * half_rows
        if depth > 0:
            at = at + bits[side][0] * quarter
        if depth > 1:
            at = at + bits[side][1] * eighth
        return at

    def z_copy(c, stage, side):
        if stage == 0:
            src = part.at[pl.ds(base_row(c, 0) + side * half_rows + (1 - bits[side][0]) * quarter, quarter)]
            dst = z1.at[c, side]
        elif stage == 1:
            src = part.at[pl.ds(base_row(c, 0) + kept(side, 1) + (1 - bits[side][1]) * eighth, eighth)]
            dst = z2.at[c, side]
        else:
            rows = eighth if stage == 2 else quarter
            src = dst = state.at[pl.ds(base_row(c, 0) + kept(side, 2 if stage == 2 else 1), rows)]
        return pltpu.make_async_remote_copy(
            src_ref=src, dst_ref=dst, send_sem=z_send.at[c, stage, side], recv_sem=z_recv.at[c, stage, side],
            device_id=(o, peers[side][stage if stage < 2 else 3 - stage]), device_id_type=MESH,
        )

    def state_copy(c):
        rows = pl.ds(base_row(c, 0), CROWS)
        return pltpu.make_async_remote_copy(
            src_ref=state.at[rows], dst_ref=state.at[rows],
            send_sem=st_send.at[c], recv_sem=st_recv.at[c],
            device_id=(o, other), device_id_type=MESH,
        )

    def reduce(stage, c):
        if stage == 0:
            core_copy(c).wait_recv()
            rows = pl.ds(base_row(c, 0), CROWS)
            part[rows, :] = part[rows, :] + core_in[c]
        else:
            for side in range(2):
                z_copy(c, stage - 1, side).wait_recv()
                if stage < 3:
                    rows = pl.ds(base_row(c, 0) + kept(side, stage), quarter if stage == 1 else eighth)
                    total = part[rows, :] + (z1, z2)[stage - 1][c, side]
                    if stage == 1:
                        part[rows, :] = total
                    else:
                        state[rows, :] = total.astype(bf16)
        if stage < 4:
            for side in range(2):
                z_copy(c, stage, side).start()
        else:
            state_copy(c).start()

    def mass_copy(seq, d):
        return pltpu.make_async_remote_copy(
            src_ref=mass.at[pl.ds(seq * HEADS, HEADS)], dst_ref=mass_in.at[seq, d],
            send_sem=mass_send.at[seq, d], recv_sem=mass_recv.at[seq, d],
            device_id=(o, lax.rem(s + d, 8)), device_id_type=MESH,
        )

    def take_mass(seq):
        for d in range(1, 8):
            mass_copy(seq, d).wait()
        rows = pl.ds(seq * HEADS, HEADS)
        total = mass[rows, :]
        for d in range(1, 8):
            total = total + mass_in[seq, d]
        mass[rows, :] = total

    def factors(seq, group):
        for j in range(HG):
            h = group * HG + j
            rows = pl.ds(h * PITCH, T)
            query = fa[rows, :].astype(bf16)
            q_head[seq * HEADS + h] = query
            m = mass[pl.ds(seq * HEADS + h, 1), :]
            bottom = jnp.sum(query.astype(f32) * m, axis=1, keepdims=True) + 0.001 * COUNT
            factor[seq, rows, :] = COUNT**0.5 / (bottom * factor[seq, rows, :])

    def read(seq, group):
        for j in range(HG):
            h = seq * HEADS + group * HG + j
            top = jnp.dot(q_head[h], state[h * D : (h + 1) * D, :], preferred_element_type=f32)
            rows = pl.ds((group * HG + j) * PITCH, T)
            q_head[h] = (top * factor[seq, rows, :]).astype(bf16)

    def out_copy(seq, slab):
        columns = pl.ds(pl.multiple_of(slab * D, D), D)
        return pltpu.make_async_copy(
            staged.at[seq, slab], out.at[seq, :, columns], out_sem.at[seq, slab]
        )

    def project(half, seq, tiles):
        total = (fa, fb)[seq]
        names = [shard(da, db) for da, db in GROUPS[half]]
        left = jnp.concatenate([q_head[seq * HEADS + name] for name in names], axis=1)
        for tile in tiles:
            columns = slice(tile * 2 * D, (tile + 1) * 2 * D)
            right = jnp.concatenate(
                [w_buf[name, :, :, :, columns].reshape(D, 2 * D) for name in names], axis=0
            )
            result = jnp.dot(left, right, preferred_element_type=f32)
            for j in range(2):
                slab = 2 * tile + j
                piece = result[:, j * D : (j + 1) * D]
                rows = pl.ds(slab * PITCH, T)
                if half == 0:
                    total[rows, :] = piece
                else:
                    staged[seq, slab] = (total[rows, :] + piece).astype(bf16)
                    out_copy(seq, slab).start()

    loaded = set()

    def need(i, seq, pieces):
        for piece in pieces:
            if (i, seq, piece) not in loaded:
                loaded.add((i, seq, piece))
                load(i, seq, piece).wait()

    steps = T // TC // 2
    per = PIECES // 2
    gathered = set()
    for token in make_plan():
        kind, args = token[0], token[1:]
        if kind in ("key", "query", "gate"):
            seq, half = args
            source = {"key": 0, "query": 2, "gate": 3}[kind]
            need(source, seq, range(half * per, (half + 1) * per))
            spread(
                natural[source], factor.at[seq] if kind == "gate" else fa, seq,
                (lambda x: 1.0 + jnp.exp(-x)) if kind == "gate" else feature,
                half * steps, (half + 1) * steps,
            )
        elif kind == "value":
            need(1, args[0], range(PIECES))
            spread(v_nat, fb, args[0], lambda x: x, 0, T // TC)
        elif kind == "heads":
            seq, group, side = args
            heads(seq, (mine if side else theirs) + 4 * group)
            if side == 0:
                core_copy(2 * seq + group).start()
        elif kind == "mass":
            for d in range(1, 8):
                mass_copy(args[0], d).start()
        elif kind == "take":
            take_mass(*args)
        elif kind == "factor":
            factors(*args)
        elif kind == "sum":
            reduce(*args)
        elif kind == "weight":
            w_arrive(*ORDER[args[0]])
        elif kind == "last":
            state_copy(*args).wait_recv()
        elif kind == "read":
            read(*args)
        else:
            half, seq, quarter_of = args
            for da, db, h in ORDER:
                if (db, da) in GROUPS[half] and (da, db, h) not in gathered:
                    gathered.add((da, db, h))
                    arrival(w_buf.at[shard(db, da), 1 - core, h], wp_sem.at[da, db, h])
            project(half, seq, range(quarter_of * 2, quarter_of * 2 + 2))

    for item in sent:
        w_copy(*item).wait_send()
    for c in range(CHUNKS):
        core_copy(c).wait_send()
        state_copy(c).wait_send()
        for stage in range(4):
            for side in range(2):
                z_copy(c, stage, side).wait_send()
    for seq in range(SEQS):
        for slab in range(HEADS):
            out_copy(seq, slab).wait()


def body(queries_in, keys_in, values_in, gate_rows, out_weight):
    any_space = pl.BlockSpec(memory_space=pl.ANY)
    natural = pltpu.VMEM((SEQS, T, HEADS, D), bf16)
    wide = pltpu.VMEM((HEADS * PITCH, D), f32)
    dma = pltpu.SemaphoreType.DMA
    return pl.pallas_call(
        attention,
        out_shape=jax.ShapeDtypeStruct((SEQS, T, WIDTH), bf16),
        in_specs=[any_space] * 5,
        out_specs=any_space,
        scratch_shapes=[
            natural, natural, natural, natural,
            wide, wide, pltpu.VMEM((SEQS, HEADS * PITCH, D), f32),
            pltpu.VMEM((SEQS * HEADS, T, D), bf16),
            pltpu.VMEM((SEQS * HEADS * D, D), f32),
            pltpu.VMEM((SEQS * HEADS, D), f32),
            pltpu.VMEM((SEQS, 8, HEADS, D), f32),
            pltpu.VMEM((CHUNKS, CROWS, D), f32),
            pltpu.VMEM((CHUNKS, 2, CROWS // 4, D), f32),
            pltpu.VMEM((CHUNKS, 2, CROWS // 8, D), f32),
            pltpu.VMEM((SEQS * HEADS * D, D), bf16),
            pltpu.VMEM((SEQS, HEADS, T, D), bf16),
            pltpu.VMEM((16, 2, 2, ROWS, WIDTH), bf16),
            dma((4, SEQS, PIECES)), dma, dma((SEQS, HEADS)),
            dma((CHUNKS,)), dma((CHUNKS,)), dma((CHUNKS, 4, 2)), dma((CHUNKS, 4, 2)),
            dma((CHUNKS,)), dma((CHUNKS,)), dma((SEQS, 8)), dma((SEQS, 8)),
            dma((5, 4, 4, 2)), dma((4, 4, 2)), dma((4, 4, 2)),
        ],
        compiler_params=pltpu.CompilerParams(
            collective_id=0, has_side_effects=True, vmem_limit_bytes=63 * 1024 * 1024
        ),
        name="attention",
    )(queries_in, keys_in, values_in, gate_rows, out_weight.reshape(2, 2, ROWS, WIDTH))


def solution(mesh):
    rows = P("outer", "span", None, None)
    return jax.shard_map(
        body, mesh=mesh, in_specs=(rows, rows, rows, rows, P("outer", None)),
        out_specs=P("outer", "span", None), check_vma=False,
    )
```

```python
import functools
import jax
import jax.numpy as jnp
from jax import lax
from jax.experimental import pallas as pl
from jax.experimental.pallas import tpu as pltpu
from jax.sharding import PartitionSpec as P

f32 = jnp.float32
bf16 = jnp.bfloat16
MESH = pl.DeviceIdType.MESH

SEQS = 2
T = 512
HEADS = 16
D = 128
WIDTH = HEADS * D
COUNT = 4096
PITCH = T + 4
TC = 64
HG = 4
PIECES = 4
ROWS = 32
BLOCKS = 8
CHUNKS = 4
CROWS = 4 * D

ORDER = (
    (3, 0, 0), (1, 0, 1), (0, 3, 0), (0, 1, 1), (3, 0, 1), (1, 0, 0), (0, 3, 1), (0, 1, 0),
    (2, 0, 0), (2, 0, 1), (3, 3, 0), (3, 1, 0), (1, 1, 1), (1, 3, 1), (0, 2, 0), (0, 2, 1),
    (3, 1, 1), (3, 3, 1), (1, 3, 0), (1, 1, 0), (2, 3, 0), (2, 1, 0), (2, 1, 1), (2, 3, 1),
    (3, 2, 0), (3, 2, 1), (1, 2, 0), (1, 2, 1), (2, 2, 0), (2, 2, 1),
)
ARRIVE = (
    5.8, 5.8, 5.8, 5.8, 8.6, 8.6, 8.6, 8.6, 11.6, 11.6, 11.6, 11.6, 13.0, 13.0, 14.4, 14.4,
    15.8, 15.8, 17.2, 17.2, 18.7, 18.7, 20.1, 20.1, 21.5, 22.9, 22.9, 22.9, 24.3, 24.5,
)
GROUPS = (
    ((0, 0), (3, 0), (1, 0), (0, 3), (0, 1), (2, 0), (0, 2), (3, 3)),
    ((3, 1), (1, 3), (1, 1), (2, 3), (3, 2), (2, 1), (1, 2), (2, 2)),
)


def make_plan():
    begin, weights_at, wire, hop = 2.5, 2.4, 1.4, 3.1
    units = []
    for seq in range(SEQS):
        for half in range(2):
            units.append((("key", seq, half), 0.47, ()))
        units.append((("value", seq), 0.35, ()))
        for side in range(2):
            for group in range(2):
                units.append((("heads", seq, group, side), 0.3, ()))
        units.append((("mass", seq), 0.05, ()))
    for seq in range(SEQS):
        for half in range(2):
            units.append((("query", seq, half), 0.47, ()))
        for half in range(2):
            units.append((("gate", seq, half), 0.4, ()))
        units.append((("take", seq), 0.15, ()))
        for group in range(4):
            units.append((("factor", seq, group), 0.35, ()))
    for seq in range(SEQS):
        for group in range(2):
            c = 2 * seq + group
            units.append((("last", c), 0.02, (("sum", 3, c),)))
        for group in range(4):
            units.append((("read", seq, group), 0.3, ()))
        for quarter in range(4):
            units.append((("project", 0, seq, quarter), 0.6, (("weight", 17),)))
    for seq in range(SEQS):
        for quarter in range(4):
            units.append((("project", 1, seq, quarter), 0.6, (("weight", 29),)))

    ready = {("weight", i): weights_at + at for i, at in enumerate(ARRIVE)}
    plan, done, clock, at, link = [], set(), begin, 0, 0.0
    while at < len(units) or ready:
        due = [e for e in ready if ready[e] <= clock]
        token = None
        if due:
            token = min(due, key=lambda e: (ready[e], e))
        elif at < len(units) and all(n in done for n in units[at][2]):
            token, cost, _ = units[at]
            at += 1
            clock += cost
            if token[0] == "heads" and token[3] == 0:
                ready["sum", 0, 2 * token[1] + token[2]] = clock + 1.6
        else:
            token = min(ready, key=lambda e: (ready[e], e))
            clock = ready[token]
        if token in ready:
            del ready[token]
            clock += 0.05 if token[0] == "weight" else (0.25, 0.15, 0.15, 0.0)[token[1]]
            if token[0] == "sum" and token[1] < 3:
                link = max(link, clock) + wire
                ready["sum", token[1] + 1, token[2]] = link + hop
        done.add(token)
        if token[:2] != ("sum", 3):
            plan.append(token)
    return plan


def feature(x):
    return jnp.maximum(x, 0.0) + jnp.exp(jnp.minimum(x, 0.0))


def spread(src, dst, seq, fn, low, high):
    def step(i, carry):
        start = i * TC
        values = fn(src[seq, pl.ds(start, TC)].astype(f32))
        for t in range(TC):
            for half in range(2):
                dst[pl.ds(start + t + 8 * half * PITCH, 8, stride=PITCH), :] = values[
                    t, 8 * half : 8 * half + 8, :
                ]
        return carry

    lax.fori_loop(low, high, step, 0)


def attention(
    q_in, k_in, v_in, g_in, w_in,
    out,
    q_nat, k_nat, v_nat, g_nat,
    fa, fb, factor, q_head, part, mass, mass_in,
    core_in, z1, z2, state, staged, w_buf,
    load_sem, w_load_sem, out_sem,
    core_send, core_recv, z_send, z_recv, st_send, st_recv, mass_send, mass_recv,
    ws_sem, wr_sem, wp_sem,
):
    o = lax.axis_index("outer")
    s = lax.axis_index("span")
    core = lax.rem(s, 2)
    z = lax.div(s, 2)
    other = s + 1 - 2 * core
    first = s + 2 * (1 - 2 * lax.rem(z, 2))
    second = 2 * (3 - z) + core
    upper = lax.div(z, 2)
    gray = lax.rem(z + upper, 2)
    sa = 1 + 3 * core
    sb = 4 - 3 * core
    a = lax.rem(lax.div(o, sa), 4)
    b = lax.rem(lax.div(o, sb), 4)

    def shard(da, db):
        return lax.rem(a + da, 4) * sa + lax.rem(b + db, 4) * sb

    arrays = (k_in, v_in, q_in, g_in)
    natural = (k_nat, v_nat, q_nat, g_nat)
    step = T // PIECES

    def load(i, seq, piece):
        rows = pl.ds(piece * step, step)
        return pltpu.make_async_copy(
            arrays[i].at[seq, rows], natural[i].at[seq, rows], load_sem.at[i, seq, piece]
        )

    own_w = pltpu.make_async_copy(w_in, w_buf.at[o], w_load_sem)
    own_w.start()
    for pair in ((0, 1), (2, 3)):
        for seq in range(SEQS):
            for i in pair:
                for piece in range(PIECES):
                    load(i, seq, piece).start()

    barrier = pltpu.get_barrier_semaphore()
    for da, db in ((1, 0), (3, 0), (0, 1), (0, 3)):
        pl.semaphore_signal(barrier, inc=1, device_id=(shard(da, db), s), device_id_type=MESH)
    for d in range(1, 8):
        pl.semaphore_signal(barrier, inc=1, device_id=(o, lax.rem(s + d, 8)), device_id_type=MESH)
    own_w.wait()
    pl.semaphore_wait(barrier, 11)

    kinds = {"A+": (1, 0), "A-": (3, 0), "B+": (0, 1), "B-": (0, 3)}
    sent = []

    def w_copy(kind, da, db, h):
        ref = w_buf.at[shard(da, db), core, h]
        if kind == "P":
            return pltpu.make_async_remote_copy(
                src_ref=ref, dst_ref=ref, send_sem=ws_sem.at[4, da, db, h], recv_sem=wp_sem.at[da, db, h],
                device_id=(o, other), device_id_type=MESH,
            )
        ka, kb = kinds[kind]
        return pltpu.make_async_remote_copy(
            src_ref=ref,
            dst_ref=ref,
            send_sem=ws_sem.at[list(kinds).index(kind), da, db, h],
            recv_sem=wr_sem.at[(da - ka) % 4, (db - kb) % 4, h],
            device_id=(shard(ka, kb), s),
            device_id_type=MESH,
        )

    def w_send(kind, da, db, h):
        w_copy(kind, da, db, h).start()
        sent.append((kind, da, db, h))

    def arrival(ref, sem):
        pltpu.make_async_remote_copy(
            src_ref=ref, dst_ref=ref, send_sem=ws_sem.at[0, 0, 0, 0], recv_sem=sem,
            device_id=(o, other), device_id_type=MESH,
        ).wait_recv()

    def w_arrive(da, db, h):
        arrival(w_buf.at[shard(da, db), core, h], wr_sem.at[da, db, h])
        if db == 0:
            if da == 3 and h == 0:
                w_send("A+", da, db, h)
            if da == 1 and h == 1:
                w_send("A-", da, db, h)
            w_send("B+", da, db, h)
            w_send("B-", da, db, h)
        elif db == 3 and h == 0:
            w_send("B+", da, db, h)
        elif db == 1 and h == 1:
            w_send("B-", da, db, h)
        w_send("P", da, db, h)

    for names, h in ((("A+", "B+"), 0), (("A-", "B-"), 1), (("A+", "B+"), 1), (("A-", "B-"), 0)):
        for name in names:
            w_send(name, 0, 0, h)

    mine = core * 8
    theirs = 8 - mine

    def heads(seq, base):
        for j in range(HG):
            h = base + j
            key = fa[pl.ds(h * PITCH, T), :].astype(bf16)
            value = fb[pl.ds(h * PITCH, T), :].astype(bf16)
            part[pl.ds((seq * HEADS + h) * D, D), :] = lax.dot_general(
                key, value, (((0,), (0,)), ((), ())), preferred_element_type=f32
            )
            m = jnp.sum(key.astype(f32).reshape(T // 8, 8, D), axis=0)
            mass[pl.ds(seq * HEADS + h, 1), :] = jnp.sum(m, axis=0, keepdims=True)

    def base_row(c, side):
        return ((c // 2) * HEADS + (theirs if side else mine) + 4 * (c % 2)) * D

    def core_copy(c):
        return pltpu.make_async_remote_copy(
            src_ref=part.at[pl.ds(base_row(c, 1), CROWS)], dst_ref=core_in.at[c],
            send_sem=core_send.at[c], recv_sem=core_recv.at[c],
            device_id=(o, other), device_id_type=MESH,
        )

    half_rows, quarter = CROWS // 2, CROWS // 4
    bits = (gray, upper)
    peers = ((first, second), (second, first))

    def quarter_row(side, keep):
        bit = bits[side] if keep else 1 - bits[side]
        return side * half_rows + bit * quarter

    def z_copy(c, stage, side):
        src = part.at[pl.ds(base_row(c, 0) + quarter_row(side, stage == 1), quarter)]
        return pltpu.make_async_remote_copy(
            src_ref=src, dst_ref=(z1, z2)[stage].at[c, side],
            send_sem=z_send.at[c, stage, side], recv_sem=z_recv.at[c, stage, side],
            device_id=(o, peers[side][stage]), device_id_type=MESH,
        )

    def state_copy(c, side, to):
        rows = pl.ds(base_row(c, 0) + quarter_row(side, True), quarter)
        peer = peers[side][0]
        return pltpu.make_async_remote_copy(
            src_ref=state.at[rows], dst_ref=state.at[rows],
            send_sem=st_send.at[c, side, to], recv_sem=st_recv.at[c, side, to],
            device_id=(o, (peer, peer + 1 - 2 * core, other)[to]), device_id_type=MESH,
        )

    def take_state(c):
        for side in range(2):
            for to in range(3):
                rows = pl.ds(base_row(c, int(to > 0)) + quarter_row(side, to == 2), quarter)
                arrival(state.at[rows], st_recv.at[c, side, to])

    def reduce(stage, c):
        if stage == 0:
            core_copy(c).wait_recv()
            rows = pl.ds(base_row(c, 0), CROWS)
            part[rows, :] = part[rows, :] + core_in[c]
            for side in range(2):
                z_copy(c, 0, side).start()
        else:
            for side in range(2):
                z_copy(c, stage - 1, side).wait_recv()
                rows = pl.ds(base_row(c, 0) + quarter_row(side, True), quarter)
                total = part[rows, :] + (z1, z2)[stage - 1][c, side]
                if stage == 1:
                    part[rows, :] = total
                    z_copy(c, 1, side).start()
                else:
                    state[rows, :] = total.astype(bf16)
                    for to in range(3):
                        state_copy(c, side, to).start()

    def mass_copy(seq, d):
        return pltpu.make_async_remote_copy(
            src_ref=mass.at[pl.ds(seq * HEADS, HEADS)], dst_ref=mass_in.at[seq, d],
            send_sem=mass_send.at[seq, d], recv_sem=mass_recv.at[seq, d],
            device_id=(o, lax.rem(s + d, 8)), device_id_type=MESH,
        )

    def take_mass(seq):
        for d in range(1, 8):
            mass_copy(seq, d).wait()
        rows = pl.ds(seq * HEADS, HEADS)
        total = mass[rows, :]
        for d in range(1, 8):
            total = total + mass_in[seq, d]
        mass[rows, :] = total

    def factors(seq, group):
        for j in range(HG):
            h = group * HG + j
            rows = pl.ds(h * PITCH, T)
            query = fa[rows, :].astype(bf16)
            q_head[seq * HEADS + h] = query
            m = mass[pl.ds(seq * HEADS + h, 1), :]
            bottom = jnp.sum(query.astype(f32) * m, axis=1, keepdims=True) + 0.001 * COUNT
            factor[seq, rows, :] = COUNT**0.5 / (bottom * factor[seq, rows, :])

    def read(seq, group):
        for j in range(HG):
            h = seq * HEADS + group * HG + j
            top = jnp.dot(q_head[h], state[h * D : (h + 1) * D, :], preferred_element_type=f32)
            rows = pl.ds((group * HG + j) * PITCH, T)
            q_head[h] = (top * factor[seq, rows, :]).astype(bf16)

    def out_copy(seq, slab):
        columns = pl.ds(pl.multiple_of(slab * D, D), D)
        return pltpu.make_async_copy(
            staged.at[seq, slab], out.at[seq, :, columns], out_sem.at[seq, slab]
        )

    def project(half, seq, tiles):
        total = (fa, fb)[seq]
        names = [shard(da, db) for da, db in GROUPS[half]]
        left = jnp.concatenate([q_head[seq * HEADS + name] for name in names], axis=1)
        for tile in tiles:
            columns = slice(tile * 2 * D, (tile + 1) * 2 * D)
            right = jnp.concatenate(
                [w_buf[name, :, :, :, columns].reshape(D, 2 * D) for name in names], axis=0
            )
            result = jnp.dot(left, right, preferred_element_type=f32)
            for j in range(2):
                slab = 2 * tile + j
                piece = result[:, j * D : (j + 1) * D]
                rows = pl.ds(slab * PITCH, T)
                if half == 0:
                    total[rows, :] = piece
                else:
                    staged[seq, slab] = (total[rows, :] + piece).astype(bf16)
                    out_copy(seq, slab).start()

    loaded = set()

    def need(i, seq, pieces):
        for piece in pieces:
            if (i, seq, piece) not in loaded:
                loaded.add((i, seq, piece))
                load(i, seq, piece).wait()

    steps = T // TC // 2
    per = PIECES // 2
    gathered = set()
    for token in make_plan():
        kind, args = token[0], token[1:]
        if kind in ("key", "query", "gate"):
            seq, half = args
            source = {"key": 0, "query": 2, "gate": 3}[kind]
            need(source, seq, range(half * per, (half + 1) * per))
            spread(
                natural[source], factor.at[seq] if kind == "gate" else fa, seq,
                (lambda x: 1.0 + jnp.exp(-x)) if kind == "gate" else feature,
                half * steps, (half + 1) * steps,
            )
        elif kind == "value":
            need(1, args[0], range(PIECES))
            spread(v_nat, fb, args[0], lambda x: x, 0, T // TC)
        elif kind == "heads":
            seq, group, side = args
            heads(seq, (mine if side else theirs) + 4 * group)
            if side == 0:
                core_copy(2 * seq + group).start()
        elif kind == "mass":
            for d in range(1, 8):
                mass_copy(args[0], d).start()
        elif kind == "take":
            take_mass(*args)
        elif kind == "factor":
            factors(*args)
        elif kind == "sum":
            reduce(*args)
        elif kind == "weight":
            w_arrive(*ORDER[args[0]])
        elif kind == "last":
            take_state(*args)
        elif kind == "read":
            read(*args)
        else:
            half, seq, quarter_of = args
            for da, db, h in ORDER:
                if (db, da) in GROUPS[half] and (da, db, h) not in gathered:
                    gathered.add((da, db, h))
                    arrival(w_buf.at[shard(db, da), 1 - core, h], wp_sem.at[da, db, h])
            project(half, seq, range(quarter_of * 2, quarter_of * 2 + 2))

    for item in sent:
        w_copy(*item).wait_send()
    for c in range(CHUNKS):
        core_copy(c).wait_send()
        for side in range(2):
            for stage in range(2):
                z_copy(c, stage, side).wait_send()
            for to in range(3):
                state_copy(c, side, to).wait_send()
    for seq in range(SEQS):
        for slab in range(HEADS):
            out_copy(seq, slab).wait()


def hand_over(src, dst, buffer, in_sem, out_sem):
    blocks = [(seq, i) for seq in range(SEQS) for i in range(BLOCKS)]
    rows = [pl.ds(i * (T // BLOCKS), T // BLOCKS) for i in range(BLOCKS)]

    def fetch(seq, i):
        return pltpu.make_async_copy(src.at[seq, rows[i]], buffer.at[seq, rows[i]], in_sem.at[seq, i])

    def put(seq, i):
        return pltpu.make_async_copy(buffer.at[seq, rows[i]], dst.at[seq, rows[i]], out_sem.at[seq, i])

    for block in blocks:
        fetch(*block).start()
    for block in blocks:
        fetch(*block).wait()
        put(*block).start()
    for block in blocks:
        put(*block).wait()


def body(queries_in, keys_in, values_in, gate_rows, out_weight):
    any_space = pl.BlockSpec(memory_space=pl.ANY)
    natural = pltpu.VMEM((SEQS, T, HEADS, D), bf16)
    wide = pltpu.VMEM((HEADS * PITCH, D), f32)
    dma = pltpu.SemaphoreType.DMA
    result = pl.pallas_call(
        attention,
        out_shape=jax.ShapeDtypeStruct((SEQS, T, WIDTH), bf16),
        in_specs=[any_space] * 5,
        out_specs=any_space,
        scratch_shapes=[
            natural, natural, natural, natural,
            wide, wide, pltpu.VMEM((SEQS, HEADS * PITCH, D), f32),
            pltpu.VMEM((SEQS * HEADS, T, D), bf16),
            pltpu.VMEM((SEQS * HEADS * D, D), f32),
            pltpu.VMEM((SEQS * HEADS, D), f32),
            pltpu.VMEM((SEQS, 8, HEADS, D), f32),
            pltpu.VMEM((CHUNKS, CROWS, D), f32),
            pltpu.VMEM((CHUNKS, 2, CROWS // 4, D), f32),
            pltpu.VMEM((CHUNKS, 2, CROWS // 4, D), f32),
            pltpu.VMEM((SEQS * HEADS * D, D), bf16),
            pltpu.VMEM((SEQS, HEADS, T, D), bf16),
            pltpu.VMEM((16, 2, 2, ROWS, WIDTH), bf16),
            dma((4, SEQS, PIECES)), dma, dma((SEQS, HEADS)),
            dma((CHUNKS,)), dma((CHUNKS,)), dma((CHUNKS, 2, 2)), dma((CHUNKS, 2, 2)),
            dma((CHUNKS, 2, 3)), dma((CHUNKS, 2, 3)), dma((SEQS, 8)), dma((SEQS, 8)),
            dma((5, 4, 4, 2)), dma((4, 4, 2)), dma((4, 4, 2)),
        ],
        compiler_params=pltpu.CompilerParams(
            collective_id=0, has_side_effects=True, vmem_limit_bytes=63 * 1024 * 1024
        ),
        name="attention",
    )(queries_in, keys_in, values_in, gate_rows, out_weight.reshape(2, 2, ROWS, WIDTH))
    return pl.pallas_call(
        hand_over,
        out_shape=jax.ShapeDtypeStruct((SEQS, T, WIDTH), bf16),
        in_specs=[any_space],
        out_specs=any_space,
        scratch_shapes=[pltpu.VMEM((SEQS, T, WIDTH), bf16), dma((SEQS, BLOCKS)), dma((SEQS, BLOCKS))],
        compiler_params=pltpu.CompilerParams(vmem_limit_bytes=63 * 1024 * 1024),
        name="hand_over",
    )(result)


def solution(mesh):
    rows = P("outer", "span", None, None)
    return jax.shard_map(
        body, mesh=mesh, in_specs=(rows, rows, rows, rows, P("outer", None)),
        out_specs=P("outer", "span", None), check_vma=False,
    )
```

```python
import functools
import jax
import jax.numpy as jnp
from jax import lax
from jax.experimental import pallas as pl
from jax.experimental.pallas import tpu as pltpu
from jax.sharding import PartitionSpec as P

f32 = jnp.float32
bf16 = jnp.bfloat16
MESH = pl.DeviceIdType.MESH

SEQS = 2
T = 512
HEADS = 16
D = 128
WIDTH = HEADS * D
COUNT = 4096
PITCH = T + 4
TC = 64
HG = 4
PIECES = 4
ROWS = 32
BLOCKS = 8
CHUNKS = 4
CROWS = 4 * D

ORDER = (
    (3, 0, 0), (1, 0, 1), (0, 3, 0), (0, 1, 1), (3, 0, 1), (1, 0, 0), (0, 3, 1), (0, 1, 0),
    (2, 0, 0), (2, 0, 1), (3, 3, 0), (3, 1, 0), (1, 1, 1), (1, 3, 1), (0, 2, 0), (0, 2, 1),
    (3, 1, 1), (3, 3, 1), (1, 3, 0), (1, 1, 0), (2, 3, 0), (2, 1, 0), (2, 1, 1), (2, 3, 1),
    (3, 2, 0), (3, 2, 1), (1, 2, 0), (1, 2, 1), (2, 2, 0), (2, 2, 1),
)
ARRIVE = (
    5.8, 5.8, 5.8, 5.8, 8.6, 8.6, 8.6, 8.6, 11.6, 11.6, 11.6, 11.6, 13.0, 13.0, 14.4, 14.4,
    15.8, 15.8, 17.2, 17.2, 18.7, 18.7, 20.1, 20.1, 21.5, 22.9, 22.9, 22.9, 24.3, 24.5,
)
GROUPS = (
    ((0, 0), (3, 0), (1, 0), (0, 3), (0, 1), (2, 0), (0, 2), (3, 3), (3, 1), (1, 3)),
    ((1, 1), (2, 3), (3, 2), (2, 1), (1, 2), (2, 2)),
)


def make_plan():
    begin, weights_at, wire, hop = 2.5, 2.4, 1.4, 3.4
    units = []
    for seq in range(SEQS):
        for half in range(2):
            units.append((("key", seq, half), 0.47, ()))
        units.append((("value", seq), 0.35, ()))
        for side in range(2):
            for group in range(2):
                units.append((("heads", seq, group, side), 0.3, ()))
        units.append((("mass", seq), 0.05, ()))
    for seq in range(SEQS):
        for half in range(2):
            units.append((("query", seq, half), 0.47, ()))
        for half in range(2):
            units.append((("gate", seq, half), 0.4, ()))
        units.append((("take", seq), 0.15, ()))
        for group in range(4):
            units.append((("factor", seq, group), 0.35, ()))
    first_work = len(units)
    for seq in range(SEQS):
        for group in range(2):
            c = 2 * seq + group
            units.append((("last", c), 0.02, (("sum", 3, c),)))
        for group in range(4):
            units.append((("read", seq, group), 0.3, (("last", 2 * seq), ("last", 2 * seq + 1))))
    for half in range(2):
        for seq in range(SEQS):
            for quarter in range(4):
                before = (("read", seq, 3),) if half == 0 else (("project", 0, seq, 3),)
                units.append((("project", half, seq, quarter), (0.75, 0.48)[half], before + (("here", half),)))

    ready = {("weight", i): weights_at + at for i, at in enumerate(ARRIVE)}
    plan, done, clock, link = [], set(), begin, 0.0
    left = list(range(len(units)))
    while left or ready:
        due = [e for e in ready if ready[e] <= clock]
        able = [i for i in left if all(n in done for n in units[i][2])]
        if left and left[0] < first_work:
            able = left[:1]
        if due:
            token = min(due, key=lambda e: (ready[e], e))
        elif able:
            left.remove(able[0])
            token, cost, _ = units[able[0]]
            clock += cost
            if token[0] == "heads" and token[3] == 0:
                ready["sum", 0, 2 * token[1] + token[2]] = clock + 1.6
        else:
            token = min(ready, key=lambda e: (ready[e], e))
            clock = ready[token]
        if token in ready:
            del ready[token]
            clock += (0.25, 0.15, 0.15, 0.0)[token[1]] if token[0] == "sum" else 0.05
            if token in (("weight", 18), ("weight", 29)):
                ready["here", int(token[1] == 29)] = clock + 1.6
            if token[0] == "sum" and token[1] < 3:
                link = max(link, clock) + wire
                ready["sum", token[1] + 1, token[2]] = link + hop
        done.add(token)
        if token[:2] != ("sum", 3) and token[0] != "here":
            plan.append(token)
    return plan


def feature(x):
    return jnp.maximum(x, 0.0) + jnp.exp(jnp.minimum(x, 0.0))


def spread(src, dst, seq, fn, low, high):
    def step(i, carry):
        start = i * TC
        values = fn(src[seq, pl.ds(start, TC)].astype(f32))
        for t in range(TC):
            for half in range(2):
                dst[pl.ds(start + t + 8 * half * PITCH, 8, stride=PITCH), :] = values[
                    t, 8 * half : 8 * half + 8, :
                ]
        return carry

    lax.fori_loop(low, high, step, 0)


def attention(
    q_in, k_in, v_in, g_in, w_in,
    out,
    q_nat, k_nat, v_nat, g_nat,
    fa, fb, factor, q_head, part, mass, mass_in,
    core_in, z1, z2, state, staged, w_buf,
    load_sem, w_load_sem, out_sem,
    core_send, core_recv, z_send, z_recv, st_send, st_recv, mass_send, mass_recv,
    ws_sem, wr_sem, wp_sem,
):
    o = lax.axis_index("outer")
    s = lax.axis_index("span")
    core = lax.rem(s, 2)
    z = lax.div(s, 2)
    other = s + 1 - 2 * core
    first = s + 2 * (1 - 2 * lax.rem(z, 2))
    second = 2 * (3 - z) + core
    upper = lax.div(z, 2)
    gray = lax.rem(z + upper, 2)
    sa = 1 + 3 * core
    sb = 4 - 3 * core
    a = lax.rem(lax.div(o, sa), 4)
    b = lax.rem(lax.div(o, sb), 4)

    def shard(da, db):
        return lax.rem(a + da, 4) * sa + lax.rem(b + db, 4) * sb

    arrays = (k_in, v_in, q_in, g_in)
    natural = (k_nat, v_nat, q_nat, g_nat)
    step = T // PIECES

    def load(i, seq, piece):
        rows = pl.ds(piece * step, step)
        return pltpu.make_async_copy(
            arrays[i].at[seq, rows], natural[i].at[seq, rows], load_sem.at[i, seq, piece]
        )

    own_w = pltpu.make_async_copy(w_in, w_buf.at[o], w_load_sem)
    own_w.start()
    for pair in ((0, 1), (2, 3)):
        for seq in range(SEQS):
            for i in pair:
                for piece in range(PIECES):
                    load(i, seq, piece).start()

    barrier = pltpu.get_barrier_semaphore()
    for da, db in ((1, 0), (3, 0), (0, 1), (0, 3)):
        pl.semaphore_signal(barrier, inc=1, device_id=(shard(da, db), s), device_id_type=MESH)
    for d in range(1, 8):
        pl.semaphore_signal(barrier, inc=1, device_id=(o, lax.rem(s + d, 8)), device_id_type=MESH)
    own_w.wait()
    pl.semaphore_wait(barrier, 11)

    kinds = {"A+": (1, 0), "A-": (3, 0), "B+": (0, 1), "B-": (0, 3)}
    sent = []

    def w_copy(kind, da, db, h):
        ref = w_buf.at[shard(da, db), core, h]
        if kind == "P":
            return pltpu.make_async_remote_copy(
                src_ref=ref, dst_ref=ref, send_sem=ws_sem.at[4, da, db, h], recv_sem=wp_sem.at[da, db, h],
                device_id=(o, other), device_id_type=MESH,
            )
        ka, kb = kinds[kind]
        return pltpu.make_async_remote_copy(
            src_ref=ref,
            dst_ref=ref,
            send_sem=ws_sem.at[list(kinds).index(kind), da, db, h],
            recv_sem=wr_sem.at[(da - ka) % 4, (db - kb) % 4, h],
            device_id=(shard(ka, kb), s),
            device_id_type=MESH,
        )

    def w_send(kind, da, db, h):
        w_copy(kind, da, db, h).start()
        sent.append((kind, da, db, h))

    def arrival(ref, sem):
        pltpu.make_async_remote_copy(
            src_ref=ref, dst_ref=ref, send_sem=ws_sem.at[0, 0, 0, 0], recv_sem=sem,
            device_id=(o, other), device_id_type=MESH,
        ).wait_recv()

    def w_arrive(da, db, h):
        arrival(w_buf.at[shard(da, db), core, h], wr_sem.at[da, db, h])
        if db == 0:
            if da == 3 and h == 0:
                w_send("A+", da, db, h)
            if da == 1 and h == 1:
                w_send("A-", da, db, h)
            w_send("B+", da, db, h)
            w_send("B-", da, db, h)
        elif db == 3 and h == 0:
            w_send("B+", da, db, h)
        elif db == 1 and h == 1:
            w_send("B-", da, db, h)
        w_send("P", da, db, h)

    for names, h in ((("A+", "B+"), 0), (("A-", "B-"), 1), (("A+", "B+"), 1), (("A-", "B-"), 0)):
        for name in names:
            w_send(name, 0, 0, h)

    mine = core * 8
    theirs = 8 - mine

    def heads(seq, base):
        for j in range(HG):
            h = base + j
            key = fa[pl.ds(h * PITCH, T), :].astype(bf16)
            value = fb[pl.ds(h * PITCH, T), :].astype(bf16)
            part[pl.ds((seq * HEADS + h) * D, D), :] = lax.dot_general(
                key, value, (((0,), (0,)), ((), ())), preferred_element_type=f32
            )
            m = jnp.sum(key.astype(f32).reshape(T // 8, 8, D), axis=0)
            mass[pl.ds(seq * HEADS + h, 1), :] = jnp.sum(m, axis=0, keepdims=True)

    def base_row(c, side):
        return ((c // 2) * HEADS + (theirs if side else mine) + 4 * (c % 2)) * D

    def core_copy(c):
        return pltpu.make_async_remote_copy(
            src_ref=part.at[pl.ds(base_row(c, 1), CROWS)], dst_ref=core_in.at[c],
            send_sem=core_send.at[c], recv_sem=core_recv.at[c],
            device_id=(o, other), device_id_type=MESH,
        )

    half_rows, quarter = CROWS // 2, CROWS // 4
    bits = (gray, upper)
    peers = ((first, second), (second, first))

    def quarter_row(side, keep):
        bit = bits[side] if keep else 1 - bits[side]
        return side * half_rows + bit * quarter

    def z_copy(c, stage, side):
        src = part.at[pl.ds(base_row(c, 0) + quarter_row(side, stage == 1), quarter)]
        return pltpu.make_async_remote_copy(
            src_ref=src, dst_ref=(z1, z2)[stage].at[c, side],
            send_sem=z_send.at[c, stage, side], recv_sem=z_recv.at[c, stage, side],
            device_id=(o, peers[side][stage]), device_id_type=MESH,
        )

    def state_copy(c, side, to):
        rows = pl.ds(base_row(c, 0) + quarter_row(side, True), quarter)
        peer = peers[side][0]
        return pltpu.make_async_remote_copy(
            src_ref=state.at[rows], dst_ref=state.at[rows],
            send_sem=st_send.at[c, side, to], recv_sem=st_recv.at[c, side, to],
            device_id=(o, (peer, peer + 1 - 2 * core, other)[to]), device_id_type=MESH,
        )

    def take_state(c):
        for side in range(2):
            for to in range(3):
                rows = pl.ds(base_row(c, int(to > 0)) + quarter_row(side, to == 2), quarter)
                arrival(state.at[rows], st_recv.at[c, side, to])

    def reduce(stage, c):
        if stage == 0:
            core_copy(c).wait_recv()
            rows = pl.ds(base_row(c, 0), CROWS)
            part[rows, :] = part[rows, :] + core_in[c]
            for side in range(2):
                z_copy(c, 0, side).start()
        else:
            for side in range(2):
                z_copy(c, stage - 1, side).wait_recv()
                rows = pl.ds(base_row(c, 0) + quarter_row(side, True), quarter)
                total = part[rows, :] + (z1, z2)[stage - 1][c, side]
                if stage == 1:
                    part[rows, :] = total
                    z_copy(c, 1, side).start()
                else:
                    state[rows, :] = total.astype(bf16)
                    for to in range(3):
                        state_copy(c, side, to).start()

    def mass_copy(seq, d):
        return pltpu.make_async_remote_copy(
            src_ref=mass.at[pl.ds(seq * HEADS, HEADS)], dst_ref=mass_in.at[seq, d],
            send_sem=mass_send.at[seq, d], recv_sem=mass_recv.at[seq, d],
            device_id=(o, lax.rem(s + d, 8)), device_id_type=MESH,
        )

    def take_mass(seq):
        for d in range(1, 8):
            mass_copy(seq, d).wait()
        rows = pl.ds(seq * HEADS, HEADS)
        total = mass[rows, :]
        for d in range(1, 8):
            total = total + mass_in[seq, d]
        mass[rows, :] = total

    def factors(seq, group):
        for j in range(HG):
            h = group * HG + j
            rows = pl.ds(h * PITCH, T)
            query = fa[rows, :].astype(bf16)
            q_head[seq * HEADS + h] = query
            m = mass[pl.ds(seq * HEADS + h, 1), :]
            bottom = jnp.sum(query.astype(f32) * m, axis=1, keepdims=True) + 0.001 * COUNT
            factor[seq, rows, :] = COUNT**0.5 / (bottom * factor[seq, rows, :])

    def read(seq, group):
        for j in range(HG):
            h = seq * HEADS + group * HG + j
            top = jnp.dot(q_head[h], state[h * D : (h + 1) * D, :], preferred_element_type=f32)
            rows = pl.ds((group * HG + j) * PITCH, T)
            q_head[h] = (top * factor[seq, rows, :]).astype(bf16)

    def out_copy(seq, slab):
        columns = pl.ds(pl.multiple_of(slab * D, D), D)
        return pltpu.make_async_copy(
            staged.at[seq, slab], out.at[seq, :, columns], out_sem.at[seq, slab]
        )

    def project(half, seq, tiles):
        total = (fa, fb)[seq]
        names = [shard(da, db) for da, db in GROUPS[half]]
        left = jnp.concatenate([q_head[seq * HEADS + name] for name in names], axis=1)
        for tile in tiles:
            columns = slice(tile * 2 * D, (tile + 1) * 2 * D)
            right = jnp.concatenate(
                [w_buf[name, :, :, :, columns].reshape(D, 2 * D) for name in names], axis=0
            )
            result = jnp.dot(left, right, preferred_element_type=f32)
            for j in range(2):
                slab = 2 * tile + j
                piece = result[:, j * D : (j + 1) * D]
                rows = pl.ds(slab * PITCH, T)
                if half == 0:
                    total[rows, :] = piece
                else:
                    staged[seq, slab] = (total[rows, :] + piece).astype(bf16)
                    out_copy(seq, slab).start()

    loaded = set()

    def need(i, seq, pieces):
        for piece in pieces:
            if (i, seq, piece) not in loaded:
                loaded.add((i, seq, piece))
                load(i, seq, piece).wait()

    steps = T // TC // 2
    per = PIECES // 2
    gathered = set()
    for token in make_plan():
        kind, args = token[0], token[1:]
        if kind in ("key", "query", "gate"):
            seq, half = args
            source = {"key": 0, "query": 2, "gate": 3}[kind]
            need(source, seq, range(half * per, (half + 1) * per))
            spread(
                natural[source], factor.at[seq] if kind == "gate" else fa, seq,
                (lambda x: 1.0 + jnp.exp(-x)) if kind == "gate" else feature,
                half * steps, (half + 1) * steps,
            )
        elif kind == "value":
            need(1, args[0], range(PIECES))
            spread(v_nat, fb, args[0], lambda x: x, 0, T // TC)
        elif kind == "heads":
            seq, group, side = args
            heads(seq, (mine if side else theirs) + 4 * group)
            if side == 0:
                core_copy(2 * seq + group).start()
        elif kind == "mass":
            for d in range(1, 8):
                mass_copy(args[0], d).start()
        elif kind == "take":
            take_mass(*args)
        elif kind == "factor":
            factors(*args)
        elif kind == "sum":
            reduce(*args)
        elif kind == "weight":
            w_arrive(*ORDER[args[0]])
        elif kind == "last":
            take_state(*args)
        elif kind == "read":
            read(*args)
        else:
            half, seq, quarter_of = args
            for da, db, h in ORDER:
                if (db, da) in GROUPS[half] and (da, db, h) not in gathered:
                    gathered.add((da, db, h))
                    arrival(w_buf.at[shard(db, da), 1 - core, h], wp_sem.at[da, db, h])
            project(half, seq, range(quarter_of * 2, quarter_of * 2 + 2))

    for item in sent:
        w_copy(*item).wait_send()
    for c in range(CHUNKS):
        core_copy(c).wait_send()
        for side in range(2):
            for stage in range(2):
                z_copy(c, stage, side).wait_send()
            for to in range(3):
                state_copy(c, side, to).wait_send()
    for seq in range(SEQS):
        for slab in range(HEADS):
            out_copy(seq, slab).wait()


def hand_over(src, dst, buffer, in_sem, out_sem):
    blocks = [(seq, i) for seq in range(SEQS) for i in range(BLOCKS)]
    rows = [pl.ds(i * (T // BLOCKS), T // BLOCKS) for i in range(BLOCKS)]

    def fetch(seq, i):
        return pltpu.make_async_copy(src.at[seq, rows[i]], buffer.at[seq, rows[i]], in_sem.at[seq, i])

    def put(seq, i):
        return pltpu.make_async_copy(buffer.at[seq, rows[i]], dst.at[seq, rows[i]], out_sem.at[seq, i])

    for block in blocks:
        fetch(*block).start()
    for block in blocks:
        fetch(*block).wait()
        put(*block).start()
    for block in blocks:
        put(*block).wait()


def body(queries_in, keys_in, values_in, gate_rows, out_weight):
    any_space = pl.BlockSpec(memory_space=pl.ANY)
    natural = pltpu.VMEM((SEQS, T, HEADS, D), bf16)
    wide = pltpu.VMEM((HEADS * PITCH, D), f32)
    dma = pltpu.SemaphoreType.DMA
    result = pl.pallas_call(
        attention,
        out_shape=jax.ShapeDtypeStruct((SEQS, T, WIDTH), bf16),
        in_specs=[any_space] * 5,
        out_specs=any_space,
        scratch_shapes=[
            natural, natural, natural, natural,
            wide, wide, pltpu.VMEM((SEQS, HEADS * PITCH, D), f32),
            pltpu.VMEM((SEQS * HEADS, T, D), bf16),
            pltpu.VMEM((SEQS * HEADS * D, D), f32),
            pltpu.VMEM((SEQS * HEADS, D), f32),
            pltpu.VMEM((SEQS, 8, HEADS, D), f32),
            pltpu.VMEM((CHUNKS, CROWS, D), f32),
            pltpu.VMEM((CHUNKS, 2, CROWS // 4, D), f32),
            pltpu.VMEM((CHUNKS, 2, CROWS // 4, D), f32),
            pltpu.VMEM((SEQS * HEADS * D, D), bf16),
            pltpu.VMEM((SEQS, HEADS, T, D), bf16),
            pltpu.VMEM((16, 2, 2, ROWS, WIDTH), bf16),
            dma((4, SEQS, PIECES)), dma, dma((SEQS, HEADS)),
            dma((CHUNKS,)), dma((CHUNKS,)), dma((CHUNKS, 2, 2)), dma((CHUNKS, 2, 2)),
            dma((CHUNKS, 2, 3)), dma((CHUNKS, 2, 3)), dma((SEQS, 8)), dma((SEQS, 8)),
            dma((5, 4, 4, 2)), dma((4, 4, 2)), dma((4, 4, 2)),
        ],
        compiler_params=pltpu.CompilerParams(
            collective_id=0, has_side_effects=True, vmem_limit_bytes=63 * 1024 * 1024
        ),
        name="attention",
    )(queries_in, keys_in, values_in, gate_rows, out_weight.reshape(2, 2, ROWS, WIDTH))
    return pl.pallas_call(
        hand_over,
        out_shape=jax.ShapeDtypeStruct((SEQS, T, WIDTH), bf16),
        in_specs=[any_space],
        out_specs=any_space,
        scratch_shapes=[pltpu.VMEM((SEQS, T, WIDTH), bf16), dma((SEQS, BLOCKS)), dma((SEQS, BLOCKS))],
        compiler_params=pltpu.CompilerParams(vmem_limit_bytes=63 * 1024 * 1024),
        name="hand_over",
    )(result)


def solution(mesh):
    rows = P("outer", "span", None, None)
    return jax.shard_map(
        body, mesh=mesh, in_specs=(rows, rows, rows, rows, P("outer", None)),
        out_specs=P("outer", "span", None), check_vma=False,
    )
```

```python
import functools
import jax
import jax.numpy as jnp
from jax import lax
from jax.experimental import pallas as pl
from jax.experimental.pallas import tpu as pltpu
from jax.sharding import PartitionSpec as P

f32 = jnp.float32
bf16 = jnp.bfloat16
MESH = pl.DeviceIdType.MESH

SEQS = 2
T = 512
HEADS = 16
D = 128
WIDTH = HEADS * D
COUNT = 4096
PITCH = T + 4
TC = 64
HG = 4
PIECES = 4
ROWS = 32
CHUNKS = 4
CROWS = 4 * D

ORDER = (
    (3, 0, 0), (1, 0, 1), (0, 3, 0), (0, 1, 1), (3, 0, 1), (1, 0, 0), (0, 3, 1), (0, 1, 0),
    (2, 0, 0), (2, 0, 1), (3, 3, 0), (3, 1, 0), (1, 1, 1), (1, 3, 1), (0, 2, 0), (0, 2, 1),
    (3, 1, 1), (3, 3, 1), (1, 3, 0), (1, 1, 0), (2, 3, 0), (2, 1, 0), (2, 1, 1), (2, 3, 1),
    (3, 2, 0), (3, 2, 1), (1, 2, 0), (1, 2, 1), (2, 2, 0), (2, 2, 1),
)
ARRIVE = (
    5.8, 5.8, 5.8, 5.8, 8.6, 8.6, 8.6, 8.6, 11.6, 11.6, 11.6, 11.6, 13.0, 13.0, 14.4, 14.4,
    15.8, 15.8, 17.2, 17.2, 18.7, 18.7, 20.1, 20.1, 21.5, 22.9, 22.9, 22.9, 24.3, 24.5,
)
GROUPS = (
    ((0, 0), (3, 0), (1, 0), (0, 3), (0, 1), (2, 0), (0, 2), (3, 3), (3, 1), (1, 3)),
    ((1, 1), (2, 3), (3, 2), (2, 1), (1, 2), (2, 2)),
)

LATE = len(GROUPS[1])


def make_plan():
    begin, weights_at, wire, hop = 2.5, 2.4, 1.4, 3.4
    units = []
    for seq in range(SEQS):
        for half in range(2):
            units.append((("key", seq, half), 0.47, ()))
        units.append((("value", seq), 0.35, ()))
        for side in range(2):
            for group in range(2):
                units.append((("heads", seq, group, side), 0.3, ()))
        units.append((("mass", seq), 0.05, ()))
    for seq in range(SEQS):
        for half in range(2):
            units.append((("query", seq, half), 0.47, ()))
        for half in range(2):
            units.append((("gate", seq, half), 0.4, ()))
        units.append((("take", seq), 0.15, ()))
        for group in range(4):
            units.append((("factor", seq, group), 0.35, ()))
    first_work = len(units)
    for seq in range(SEQS):
        for group in range(2):
            c = 2 * seq + group
            units.append((("last", c), 0.02, (("sum", 3, c),)))
        for group in range(4):
            units.append((("read", seq, group), 0.3, (("last", 2 * seq), ("last", 2 * seq + 1))))
    for seq in range(SEQS):
        for quarter in range(4):
            units.append((("project", seq, quarter), 0.75, (("read", seq, 3), ("here", 0))))

    ready = {("weight", i): weights_at + at for i, at in enumerate(ARRIVE)}
    plan, done, clock, link = [], set(), begin, 0.0
    left = list(range(len(units)))
    while left or ready:
        due = [e for e in ready if ready[e] <= clock]
        able = [i for i in left if all(n in done for n in units[i][2])]
        if left and left[0] < first_work:
            able = left[:1]
        if due:
            token = min(due, key=lambda e: (ready[e], e))
        elif able:
            left.remove(able[0])
            token, cost, _ = units[able[0]]
            clock += cost
            if token[0] == "heads" and token[3] == 0:
                ready["sum", 0, 2 * token[1] + token[2]] = clock + 1.6
        else:
            token = min(ready, key=lambda e: (ready[e], e))
            clock = ready[token]
        if token in ready:
            del ready[token]
            clock += (0.25, 0.15, 0.15, 0.0)[token[1]] if token[0] == "sum" else 0.05
            if token == ("weight", 18):
                ready["here", 0] = clock + 1.6
            if token[0] == "sum" and token[1] < 3:
                link = max(link, clock) + wire
                ready["sum", token[1] + 1, token[2]] = link + hop
        done.add(token)
        if token[:2] != ("sum", 3) and token[0] != "here":
            plan.append(token)
    return plan


def feature(x):
    return jnp.maximum(x, 0.0) + jnp.exp(jnp.minimum(x, 0.0))


def spread(src, dst, seq, fn, low, high):
    def step(i, carry):
        start = i * TC
        values = fn(src[seq, pl.ds(start, TC)].astype(f32))
        for t in range(TC):
            for half in range(2):
                dst[pl.ds(start + t + 8 * half * PITCH, 8, stride=PITCH), :] = values[
                    t, 8 * half : 8 * half + 8, :
                ]
        return carry

    lax.fori_loop(low, high, step, 0)


def attention(
    q_in, k_in, v_in, g_in, w_in,
    sum_out, mixed_out, w_out,
    q_nat, k_nat, v_nat, g_nat,
    fa, fb, factor, q_head, part, mass, mass_in,
    core_in, z1, z2, state, w_buf,
    load_sem, w_load_sem, sum_sem, mixed_sem, w_out_sem,
    core_send, core_recv, z_send, z_recv, st_send, st_recv, mass_send, mass_recv,
    ws_sem, wr_sem, wp_sem,
):
    o = lax.axis_index("outer")
    s = lax.axis_index("span")
    core = lax.rem(s, 2)
    z = lax.div(s, 2)
    other = s + 1 - 2 * core
    first = s + 2 * (1 - 2 * lax.rem(z, 2))
    second = 2 * (3 - z) + core
    upper = lax.div(z, 2)
    gray = lax.rem(z + upper, 2)
    sa = 1 + 3 * core
    sb = 4 - 3 * core
    a = lax.rem(lax.div(o, sa), 4)
    b = lax.rem(lax.div(o, sb), 4)

    def shard(da, db):
        return lax.rem(a + da, 4) * sa + lax.rem(b + db, 4) * sb

    arrays = (k_in, v_in, q_in, g_in)
    natural = (k_nat, v_nat, q_nat, g_nat)
    step = T // PIECES

    def load(i, seq, piece):
        rows = pl.ds(piece * step, step)
        return pltpu.make_async_copy(
            arrays[i].at[seq, rows], natural[i].at[seq, rows], load_sem.at[i, seq, piece]
        )

    own_w = pltpu.make_async_copy(w_in, w_buf.at[o], w_load_sem)
    own_w.start()
    for pair in ((0, 1), (2, 3)):
        for seq in range(SEQS):
            for i in pair:
                for piece in range(PIECES):
                    load(i, seq, piece).start()

    barrier = pltpu.get_barrier_semaphore()
    for da, db in ((1, 0), (3, 0), (0, 1), (0, 3)):
        pl.semaphore_signal(barrier, inc=1, device_id=(shard(da, db), s), device_id_type=MESH)
    for d in range(1, 8):
        pl.semaphore_signal(barrier, inc=1, device_id=(o, lax.rem(s + d, 8)), device_id_type=MESH)
    own_w.wait()
    pl.semaphore_wait(barrier, 11)

    kinds = {"A+": (1, 0), "A-": (3, 0), "B+": (0, 1), "B-": (0, 3)}
    sent = []

    def w_copy(kind, da, db, h):
        ref = w_buf.at[shard(da, db), core, h]
        if kind == "P":
            return pltpu.make_async_remote_copy(
                src_ref=ref, dst_ref=ref, send_sem=ws_sem.at[4, da, db, h], recv_sem=wp_sem.at[da, db, h],
                device_id=(o, other), device_id_type=MESH,
            )
        ka, kb = kinds[kind]
        return pltpu.make_async_remote_copy(
            src_ref=ref,
            dst_ref=ref,
            send_sem=ws_sem.at[list(kinds).index(kind), da, db, h],
            recv_sem=wr_sem.at[(da - ka) % 4, (db - kb) % 4, h],
            device_id=(shard(ka, kb), s),
            device_id_type=MESH,
        )

    def w_send(kind, da, db, h):
        w_copy(kind, da, db, h).start()
        sent.append((kind, da, db, h))

    def arrival(ref, sem):
        pltpu.make_async_remote_copy(
            src_ref=ref, dst_ref=ref, send_sem=ws_sem.at[0, 0, 0, 0], recv_sem=sem,
            device_id=(o, other), device_id_type=MESH,
        ).wait_recv()

    def w_arrive(da, db, h):
        arrival(w_buf.at[shard(da, db), core, h], wr_sem.at[da, db, h])
        if db == 0:
            if da == 3 and h == 0:
                w_send("A+", da, db, h)
            if da == 1 and h == 1:
                w_send("A-", da, db, h)
            w_send("B+", da, db, h)
            w_send("B-", da, db, h)
        elif db == 3 and h == 0:
            w_send("B+", da, db, h)
        elif db == 1 and h == 1:
            w_send("B-", da, db, h)
        w_send("P", da, db, h)
        if (da, db) in GROUPS[1]:
            w_store(GROUPS[1].index((da, db)), core, h, 0).start()

    def w_store(i, c, h, which):
        return pltpu.make_async_copy(
            w_buf.at[shard(*GROUPS[1][i]), c, h], w_out.at[i, c, h], w_out_sem.at[i, h, which]
        )

    for names, h in ((("A+", "B+"), 0), (("A-", "B-"), 1), (("A+", "B+"), 1), (("A-", "B-"), 0)):
        for name in names:
            w_send(name, 0, 0, h)

    mine = core * 8
    theirs = 8 - mine

    def heads(seq, base):
        for j in range(HG):
            h = base + j
            key = fa[pl.ds(h * PITCH, T), :].astype(bf16)
            value = fb[pl.ds(h * PITCH, T), :].astype(bf16)
            part[pl.ds((seq * HEADS + h) * D, D), :] = lax.dot_general(
                key, value, (((0,), (0,)), ((), ())), preferred_element_type=f32
            )
            m = jnp.sum(key.astype(f32).reshape(T // 8, 8, D), axis=0)
            mass[pl.ds(seq * HEADS + h, 1), :] = jnp.sum(m, axis=0, keepdims=True)

    def base_row(c, side):
        return ((c // 2) * HEADS + (theirs if side else mine) + 4 * (c % 2)) * D

    def core_copy(c):
        return pltpu.make_async_remote_copy(
            src_ref=part.at[pl.ds(base_row(c, 1), CROWS)], dst_ref=core_in.at[c],
            send_sem=core_send.at[c], recv_sem=core_recv.at[c],
            device_id=(o, other), device_id_type=MESH,
        )

    half_rows, quarter = CROWS // 2, CROWS // 4
    bits = (gray, upper)
    peers = ((first, second), (second, first))

    def quarter_row(side, keep):
        bit = bits[side] if keep else 1 - bits[side]
        return side * half_rows + bit * quarter

    def z_copy(c, stage, side):
        src = part.at[pl.ds(base_row(c, 0) + quarter_row(side, stage == 1), quarter)]
        return pltpu.make_async_remote_copy(
            src_ref=src, dst_ref=(z1, z2)[stage].at[c, side],
            send_sem=z_send.at[c, stage, side], recv_sem=z_recv.at[c, stage, side],
            device_id=(o, peers[side][stage]), device_id_type=MESH,
        )

    def state_copy(c, side, to):
        rows = pl.ds(base_row(c, 0) + quarter_row(side, True), quarter)
        peer = peers[side][0]
        return pltpu.make_async_remote_copy(
            src_ref=state.at[rows], dst_ref=state.at[rows],
            send_sem=st_send.at[c, side, to], recv_sem=st_recv.at[c, side, to],
            device_id=(o, (peer, peer + 1 - 2 * core, other)[to]), device_id_type=MESH,
        )

    def take_state(c):
        for side in range(2):
            for to in range(3):
                rows = pl.ds(base_row(c, int(to > 0)) + quarter_row(side, to == 2), quarter)
                arrival(state.at[rows], st_recv.at[c, side, to])

    def reduce(stage, c):
        if stage == 0:
            core_copy(c).wait_recv()
            rows = pl.ds(base_row(c, 0), CROWS)
            part[rows, :] = part[rows, :] + core_in[c]
            for side in range(2):
                z_copy(c, 0, side).start()
        else:
            for side in range(2):
                z_copy(c, stage - 1, side).wait_recv()
                rows = pl.ds(base_row(c, 0) + quarter_row(side, True), quarter)
                total = part[rows, :] + (z1, z2)[stage - 1][c, side]
                if stage == 1:
                    part[rows, :] = total
                    z_copy(c, 1, side).start()
                else:
                    state[rows, :] = total.astype(bf16)
                    for to in range(3):
                        state_copy(c, side, to).start()

    def mass_copy(seq, d):
        return pltpu.make_async_remote_copy(
            src_ref=mass.at[pl.ds(seq * HEADS, HEADS)], dst_ref=mass_in.at[seq, d],
            send_sem=mass_send.at[seq, d], recv_sem=mass_recv.at[seq, d],
            device_id=(o, lax.rem(s + d, 8)), device_id_type=MESH,
        )

    def take_mass(seq):
        for d in range(1, 8):
            mass_copy(seq, d).wait()
        rows = pl.ds(seq * HEADS, HEADS)
        total = mass[rows, :]
        for d in range(1, 8):
            total = total + mass_in[seq, d]
        mass[rows, :] = total

    def factors(seq, group):
        for j in range(HG):
            h = group * HG + j
            rows = pl.ds(h * PITCH, T)
            query = fa[rows, :].astype(bf16)
            q_head[seq * HEADS + h] = query
            m = mass[pl.ds(seq * HEADS + h, 1), :]
            bottom = jnp.sum(query.astype(f32) * m, axis=1, keepdims=True) + 0.001 * COUNT
            factor[seq, rows, :] = COUNT**0.5 / (bottom * factor[seq, rows, :])

    def read(seq, group):
        for j in range(HG):
            h = seq * HEADS + group * HG + j
            top = jnp.dot(q_head[h], state[h * D : (h + 1) * D, :], preferred_element_type=f32)
            rows = pl.ds((group * HG + j) * PITCH, T)
            q_head[h] = (top * factor[seq, rows, :]).astype(bf16)

    def mixed_copy(seq, i):
        return pltpu.make_async_copy(
            q_head.at[seq * HEADS + shard(*GROUPS[1][i])], mixed_out.at[seq, i], mixed_sem.at[seq, i]
        )

    def sum_copy(seq, slab):
        return pltpu.make_async_copy(
            (fa, fb)[seq].at[pl.ds(slab * PITCH, T)], sum_out.at[seq, slab], sum_sem.at[seq, slab]
        )

    def project(seq, tiles):
        total = (fa, fb)[seq]
        names = [shard(da, db) for da, db in GROUPS[0]]
        left = jnp.concatenate([q_head[seq * HEADS + name] for name in names], axis=1)
        for tile in tiles:
            columns = slice(tile * 2 * D, (tile + 1) * 2 * D)
            right = jnp.concatenate(
                [w_buf[name, :, :, :, columns].reshape(D, 2 * D) for name in names], axis=0
            )
            result = jnp.dot(left, right, preferred_element_type=f32)
            for j in range(2):
                slab = 2 * tile + j
                total[pl.ds(slab * PITCH, T), :] = result[:, j * D : (j + 1) * D]
                sum_copy(seq, slab).start()

    loaded = set()

    def need(i, seq, pieces):
        for piece in pieces:
            if (i, seq, piece) not in loaded:
                loaded.add((i, seq, piece))
                load(i, seq, piece).wait()

    steps = T // TC // 2
    per = PIECES // 2
    gathered = set()

    def from_other_core(group):
        for da, db, h in ORDER:
            place = (db, da)
            if place in GROUPS[group] and (da, db, h) not in gathered:
                gathered.add((da, db, h))
                arrival(w_buf.at[shard(*place), 1 - core, h], wp_sem.at[da, db, h])
                if group == 1:
                    w_store(GROUPS[1].index(place), 1 - core, h, 1).start()

    for token in make_plan():
        kind, args = token[0], token[1:]
        if kind in ("key", "query", "gate"):
            seq, half = args
            source = {"key": 0, "query": 2, "gate": 3}[kind]
            need(source, seq, range(half * per, (half + 1) * per))
            spread(
                natural[source], factor.at[seq] if kind == "gate" else fa, seq,
                (lambda x: 1.0 + jnp.exp(-x)) if kind == "gate" else feature,
                half * steps, (half + 1) * steps,
            )
        elif kind == "value":
            need(1, args[0], range(PIECES))
            spread(v_nat, fb, args[0], lambda x: x, 0, T // TC)
        elif kind == "heads":
            seq, group, side = args
            heads(seq, (mine if side else theirs) + 4 * group)
            if side == 0:
                core_copy(2 * seq + group).start()
        elif kind == "mass":
            for d in range(1, 8):
                mass_copy(args[0], d).start()
        elif kind == "take":
            take_mass(*args)
        elif kind == "factor":
            factors(*args)
        elif kind == "sum":
            reduce(*args)
        elif kind == "weight":
            w_arrive(*ORDER[args[0]])
        elif kind == "last":
            take_state(*args)
        elif kind == "read":
            read(*args)
            if args[1] == HEADS // HG - 1:
                for i in range(LATE):
                    mixed_copy(args[0], i).start()
        else:
            seq, quarter_of = args
            from_other_core(0)
            project(seq, range(quarter_of * 2, quarter_of * 2 + 2))
    from_other_core(1)

    for item in sent:
        w_copy(*item).wait_send()
    for c in range(CHUNKS):
        core_copy(c).wait_send()
        for side in range(2):
            for stage in range(2):
                z_copy(c, stage, side).wait_send()
            for to in range(3):
                state_copy(c, side, to).wait_send()
    for seq in range(SEQS):
        for slab in range(HEADS):
            sum_copy(seq, slab).wait()
        for i in range(LATE):
            mixed_copy(seq, i).wait()
    for i in range(LATE):
        for h in range(2):
            w_store(i, core, h, 0).wait()
            w_store(i, 1 - core, h, 1).wait()


def finish(sums, mixed, weight, out, sum_buf, mixed_buf, w_buf, staged, sum_sem, mixed_sem, w_sem, out_sem):
    def take_w(i):
        return pltpu.make_async_copy(weight.at[i], w_buf.at[i], w_sem.at[i])

    def take_mixed(seq):
        return pltpu.make_async_copy(mixed.at[seq], mixed_buf.at[seq], mixed_sem.at[seq])

    def take_sum(seq, slab):
        return pltpu.make_async_copy(sums.at[seq, slab], sum_buf.at[seq, slab], sum_sem.at[seq, slab])

    def put(seq, slab):
        columns = pl.ds(slab * D, D)
        return pltpu.make_async_copy(staged.at[seq, slab], out.at[seq, :, columns], out_sem.at[seq, slab])

    for i in range(LATE):
        take_w(i).start()
    for seq in range(SEQS):
        take_mixed(seq).start()
        for slab in range(HEADS):
            take_sum(seq, slab).start()
    for i in range(LATE):
        take_w(i).wait()
    for seq in range(SEQS):
        take_mixed(seq).wait()
        left = jnp.concatenate([mixed_buf[seq, i] for i in range(LATE)], axis=1)
        for tile in range(HEADS // 2):
            columns = slice(tile * 2 * D, (tile + 1) * 2 * D)
            right = w_buf[:, :, :, :, columns].reshape(LATE * D, 2 * D)
            result = jnp.dot(left, right, preferred_element_type=f32)
            for j in range(2):
                slab = 2 * tile + j
                take_sum(seq, slab).wait()
                staged[seq, slab] = (sum_buf[seq, slab] + result[:, j * D : (j + 1) * D]).astype(bf16)
                put(seq, slab).start()
    for seq in range(SEQS):
        for slab in range(HEADS):
            put(seq, slab).wait()


def body(queries_in, keys_in, values_in, gate_rows, out_weight):
    any_space = pl.BlockSpec(memory_space=pl.ANY)
    natural = pltpu.VMEM((SEQS, T, HEADS, D), bf16)
    wide = pltpu.VMEM((HEADS * PITCH, D), f32)
    dma = pltpu.SemaphoreType.DMA
    shapes = (
        ((SEQS, HEADS, T, D), f32),
        ((SEQS, LATE, T, D), bf16),
        ((LATE, 2, 2, ROWS, WIDTH), bf16),
    )
    late = pl.pallas_call(
        attention,
        out_shape=tuple(jax.ShapeDtypeStruct(*shape) for shape in shapes),
        in_specs=[any_space] * 5,
        out_specs=(any_space,) * 3,
        scratch_shapes=[
            natural, natural, natural, natural,
            wide, wide, pltpu.VMEM((SEQS, HEADS * PITCH, D), f32),
            pltpu.VMEM((SEQS * HEADS, T, D), bf16),
            pltpu.VMEM((SEQS * HEADS * D, D), f32),
            pltpu.VMEM((SEQS * HEADS, D), f32),
            pltpu.VMEM((SEQS, 8, HEADS, D), f32),
            pltpu.VMEM((CHUNKS, CROWS, D), f32),
            pltpu.VMEM((CHUNKS, 2, CROWS // 4, D), f32),
            pltpu.VMEM((CHUNKS, 2, CROWS // 4, D), f32),
            pltpu.VMEM((SEQS * HEADS * D, D), bf16),
            pltpu.VMEM((16, 2, 2, ROWS, WIDTH), bf16),
            dma((4, SEQS, PIECES)), dma, dma((SEQS, HEADS)), dma((SEQS, LATE)), dma((LATE, 2, 2)),
            dma((CHUNKS,)), dma((CHUNKS,)), dma((CHUNKS, 2, 2)), dma((CHUNKS, 2, 2)),
            dma((CHUNKS, 2, 3)), dma((CHUNKS, 2, 3)), dma((SEQS, 8)), dma((SEQS, 8)),
            dma((5, 4, 4, 2)), dma((4, 4, 2)), dma((4, 4, 2)),
        ],
        compiler_params=pltpu.CompilerParams(
            collective_id=0, has_side_effects=True, vmem_limit_bytes=63 * 1024 * 1024
        ),
        name="attention",
    )(queries_in, keys_in, values_in, gate_rows, out_weight.reshape(2, 2, ROWS, WIDTH))
    return pl.pallas_call(
        finish,
        out_shape=jax.ShapeDtypeStruct((SEQS, T, WIDTH), bf16),
        in_specs=[any_space] * 3,
        out_specs=any_space,
        scratch_shapes=[pltpu.VMEM(*shape) for shape in shapes] + [
            pltpu.VMEM((SEQS, HEADS, T, D), bf16),
            dma((SEQS, HEADS)), dma((SEQS,)), dma((LATE,)), dma((SEQS, HEADS)),
        ],
        compiler_params=pltpu.CompilerParams(vmem_limit_bytes=63 * 1024 * 1024),
        name="finish",
    )(*late)


def solution(mesh):
    rows = P("outer", "span", None, None)
    return jax.shard_map(
        body, mesh=mesh, in_specs=(rows, rows, rows, rows, P("outer", None)),
        out_specs=P("outer", "span", None), check_vma=False,
    )
```

```python
import functools
import jax
import jax.numpy as jnp
from jax import lax
from jax.experimental import pallas as pl
from jax.experimental.pallas import tpu as pltpu
from jax.sharding import PartitionSpec as P

f32 = jnp.float32
bf16 = jnp.bfloat16
MESH = pl.DeviceIdType.MESH

SEQS = 2
T = 512
HEADS = 16
D = 128
WIDTH = HEADS * D
COUNT = 4096
PITCH = T + 4
TC = 32
HG = 2
PIECES = 4
ROWS = 32
CHUNKS = 4
CROWS = 4 * D

ORDER = (
    (3, 0, 0), (1, 0, 1), (0, 3, 0), (0, 1, 1), (3, 0, 1), (1, 0, 0), (0, 3, 1), (0, 1, 0),
    (2, 0, 0), (2, 0, 1), (3, 3, 0), (3, 1, 0), (1, 1, 1), (1, 3, 1), (0, 2, 0), (0, 2, 1),
    (3, 1, 1), (3, 3, 1), (1, 3, 0), (1, 1, 0), (2, 3, 0), (2, 1, 0), (2, 1, 1), (2, 3, 1),
    (3, 2, 0), (3, 2, 1), (1, 2, 0), (1, 2, 1), (2, 2, 0), (2, 2, 1),
)
ARRIVE = (
    5.8, 5.8, 5.8, 5.8, 8.6, 8.6, 8.6, 8.6, 11.6, 11.6, 11.6, 11.6, 13.0, 13.0, 14.4, 14.4,
    15.8, 15.8, 17.2, 17.2, 18.7, 18.7, 20.1, 20.1, 21.5, 22.9, 22.9, 22.9, 24.3, 24.5,
)
GROUPS = (
    ((0, 0), (3, 0), (1, 0), (0, 3), (0, 1), (2, 0), (0, 2), (3, 3), (3, 1), (1, 3)),
    ((1, 1), (2, 3), (3, 2), (2, 1), (1, 2), (2, 2)),
)

LATE = len(GROUPS[1])


def make_plan():
    begin, weights_at, wire, hop = 2.5, 2.4, 1.4, 3.4
    units = []
    for seq in range(SEQS):
        for half in range(2):
            units.append((("key", seq, half), 0.47, ()))
        units.append((("value", seq), 0.35, ()))
        for side in range(2):
            for group in range(2):
                units.append((("heads", seq, group, side), 0.3, ()))
        units.append((("mass", seq), 0.05, ()))
    for seq in range(SEQS):
        for half in range(2):
            units.append((("query", seq, half), 0.47, ()))
        for half in range(2):
            units.append((("gate", seq, half), 0.4, ()))
        units.append((("take", seq), 0.15, ()))
        for group in range(2):
            units.append((("factor", seq, group), 0.7, ()))
    first_work = len(units)
    for seq in range(SEQS):
        for group in range(2):
            c = 2 * seq + group
            units.append((("last", c), 0.02, (("sum", 3, c),)))
        for group in range(2):
            units.append((("read", seq, group), 0.6, (("last", 2 * seq), ("last", 2 * seq + 1))))
    for seq in range(SEQS):
        for half in range(2):
            units.append((("project", seq, half), 1.5, (("read", seq, 1), ("here", 0))))

    ready = {("weight", i): weights_at + at for i, at in enumerate(ARRIVE)}
    plan, done, clock, link = [], set(), begin, 0.0
    left = list(range(len(units)))
    while left or ready:
        due = [e for e in ready if ready[e] <= clock]
        able = [i for i in left if all(n in done for n in units[i][2])]
        if left and left[0] < first_work:
            able = left[:1]
        if due:
            token = min(due, key=lambda e: (ready[e], e))
        elif able:
            left.remove(able[0])
            token, cost, _ = units[able[0]]
            clock += cost
            if token[0] == "heads" and token[3] == 0:
                ready["sum", 0, 2 * token[1] + token[2]] = clock + 1.6
        else:
            token = min(ready, key=lambda e: (ready[e], e))
            clock = ready[token]
        if token in ready:
            del ready[token]
            clock += (0.25, 0.15, 0.15, 0.0)[token[1]] if token[0] == "sum" else 0.05
            if token == ("weight", 18):
                ready["here", 0] = clock + 1.6
            if token[0] == "sum" and token[1] < 3:
                link = max(link, clock) + wire
                ready["sum", token[1] + 1, token[2]] = link + hop
        done.add(token)
        if token[:2] != ("sum", 3) and token[0] != "here":
            plan.append(token)
    return plan


def feature(x):
    return jnp.maximum(x, 0.0) + jnp.exp(jnp.minimum(x, 0.0))


def spread(src, dst, seq, fn, low, high):
    def step(i, carry):
        start = i * TC
        values = fn(src[seq, pl.ds(start, TC)].astype(f32))
        for t in range(TC):
            for half in range(2):
                dst[pl.ds(start + t + 8 * half * PITCH, 8, stride=PITCH), :] = values[
                    t, 8 * half : 8 * half + 8, :
                ]
        return carry

    lax.fori_loop(low, high, step, 0)


def attention(
    q_in, k_in, v_in, g_in, w_in,
    sum_out, mixed_out, w_out,
    q_nat, k_nat, v_nat, g_nat,
    fa, fb, factor, q_head, part, mass, mass_in,
    core_in, z1, z2, state, w_buf,
    load_sem, w_load_sem, sum_sem, mixed_sem, w_out_sem,
    core_send, core_recv, z_send, z_recv, st_send, st_recv, mass_send, mass_recv,
    ws_sem, wr_sem, wp_sem,
):
    o = lax.axis_index("outer")
    s = lax.axis_index("span")
    core = lax.rem(s, 2)
    z = lax.div(s, 2)
    other = s + 1 - 2 * core
    first = s + 2 * (1 - 2 * lax.rem(z, 2))
    second = 2 * (3 - z) + core
    upper = lax.div(z, 2)
    gray = lax.rem(z + upper, 2)
    sa = 1 + 3 * core
    sb = 4 - 3 * core
    a = lax.rem(lax.div(o, sa), 4)
    b = lax.rem(lax.div(o, sb), 4)

    def shard(da, db):
        return lax.rem(a + da, 4) * sa + lax.rem(b + db, 4) * sb

    arrays = (k_in, v_in, q_in, g_in)
    natural = (k_nat, v_nat, q_nat, g_nat)
    step = T // PIECES

    def load(i, seq, piece):
        rows = pl.ds(piece * step, step)
        return pltpu.make_async_copy(
            arrays[i].at[seq, rows], natural[i].at[seq, rows], load_sem.at[i, seq, piece]
        )

    own_w = pltpu.make_async_copy(w_in, w_buf.at[o], w_load_sem)
    own_w.start()
    for pair in ((0, 1), (2, 3)):
        for seq in range(SEQS):
            for i in pair:
                for piece in range(PIECES):
                    load(i, seq, piece).start()

    barrier = pltpu.get_barrier_semaphore()
    for da, db in ((1, 0), (3, 0), (0, 1), (0, 3)):
        pl.semaphore_signal(barrier, inc=1, device_id=(shard(da, db), s), device_id_type=MESH)
    for d in range(1, 8):
        pl.semaphore_signal(barrier, inc=1, device_id=(o, lax.rem(s + d, 8)), device_id_type=MESH)
    own_w.wait()
    pl.semaphore_wait(barrier, 11)

    kinds = {"A+": (1, 0), "A-": (3, 0), "B+": (0, 1), "B-": (0, 3)}
    sent = []

    def w_copy(kind, da, db, h):
        ref = w_buf.at[shard(da, db), core, h]
        if kind == "P":
            return pltpu.make_async_remote_copy(
                src_ref=ref, dst_ref=ref, send_sem=ws_sem.at[4, da, db, h], recv_sem=wp_sem.at[da, db, h],
                device_id=(o, other), device_id_type=MESH,
            )
        ka, kb = kinds[kind]
        return pltpu.make_async_remote_copy(
            src_ref=ref,
            dst_ref=ref,
            send_sem=ws_sem.at[list(kinds).index(kind), da, db, h],
            recv_sem=wr_sem.at[(da - ka) % 4, (db - kb) % 4, h],
            device_id=(shard(ka, kb), s),
            device_id_type=MESH,
        )

    def w_send(kind, da, db, h):
        w_copy(kind, da, db, h).start()
        sent.append((kind, da, db, h))

    def arrival(ref, sem):
        pltpu.make_async_remote_copy(
            src_ref=ref, dst_ref=ref, send_sem=ws_sem.at[0, 0, 0, 0], recv_sem=sem,
            device_id=(o, other), device_id_type=MESH,
        ).wait_recv()

    def w_arrive(da, db, h):
        arrival(w_buf.at[shard(da, db), core, h], wr_sem.at[da, db, h])
        if db == 0:
            if da == 3 and h == 0:
                w_send("A+", da, db, h)
            if da == 1 and h == 1:
                w_send("A-", da, db, h)
            w_send("B+", da, db, h)
            w_send("B-", da, db, h)
        elif db == 3 and h == 0:
            w_send("B+", da, db, h)
        elif db == 1 and h == 1:
            w_send("B-", da, db, h)
        w_send("P", da, db, h)
        if (da, db) in GROUPS[1]:
            w_store(GROUPS[1].index((da, db)), core, h, 0).start()

    def w_store(i, c, h, which):
        return pltpu.make_async_copy(
            w_buf.at[shard(*GROUPS[1][i]), c, h], w_out.at[i, c, h], w_out_sem.at[i, h, which]
        )

    for names, h in ((("A+", "B+"), 0), (("A-", "B-"), 1), (("A+", "B+"), 1), (("A-", "B-"), 0)):
        for name in names:
            w_send(name, 0, 0, h)

    mine = core * 8
    theirs = 8 - mine

    def in_steps(count, one):
        def body(i, carry):
            for j in range(HG):
                one(i * HG + j)
            return carry

        lax.fori_loop(0, count // HG, body, 0)

    def heads(seq, base):
        def one(i):
            h = base + i
            key = fa[pl.ds(h * PITCH, T), :].astype(bf16)
            value = fb[pl.ds(h * PITCH, T), :].astype(bf16)
            part[pl.ds((seq * HEADS + h) * D, D), :] = lax.dot_general(
                key, value, (((0,), (0,)), ((), ())), preferred_element_type=f32
            )
            m = jnp.sum(key.astype(f32).reshape(T // 8, 8, D), axis=0)
            mass[pl.ds(seq * HEADS + h, 1), :] = jnp.sum(m, axis=0, keepdims=True)

        in_steps(4, one)

    def base_row(c, side):
        return ((c // 2) * HEADS + (theirs if side else mine) + 4 * (c % 2)) * D

    def core_copy(c):
        return pltpu.make_async_remote_copy(
            src_ref=part.at[pl.ds(base_row(c, 1), CROWS)], dst_ref=core_in.at[c],
            send_sem=core_send.at[c], recv_sem=core_recv.at[c],
            device_id=(o, other), device_id_type=MESH,
        )

    half_rows, quarter = CROWS // 2, CROWS // 4
    bits = (gray, upper)
    peers = ((first, second), (second, first))

    def quarter_row(side, keep):
        bit = bits[side] if keep else 1 - bits[side]
        return side * half_rows + bit * quarter

    def z_copy(c, stage, side):
        src = part.at[pl.ds(base_row(c, 0) + quarter_row(side, stage == 1), quarter)]
        return pltpu.make_async_remote_copy(
            src_ref=src, dst_ref=(z1, z2)[stage].at[c, side],
            send_sem=z_send.at[c, stage, side], recv_sem=z_recv.at[c, stage, side],
            device_id=(o, peers[side][stage]), device_id_type=MESH,
        )

    def state_copy(c, side, to):
        rows = pl.ds(base_row(c, 0) + quarter_row(side, True), quarter)
        peer = peers[side][0]
        return pltpu.make_async_remote_copy(
            src_ref=state.at[rows], dst_ref=state.at[rows],
            send_sem=st_send.at[c, side, to], recv_sem=st_recv.at[c, side, to],
            device_id=(o, (peer, peer + 1 - 2 * core, other)[to]), device_id_type=MESH,
        )

    def take_state(c):
        for side in range(2):
            for to in range(3):
                rows = pl.ds(base_row(c, int(to > 0)) + quarter_row(side, to == 2), quarter)
                arrival(state.at[rows], st_recv.at[c, side, to])

    def reduce(stage, c):
        if stage == 0:
            core_copy(c).wait_recv()
            rows = pl.ds(base_row(c, 0), CROWS)
            part[rows, :] = part[rows, :] + core_in[c]
            for side in range(2):
                z_copy(c, 0, side).start()
        else:
            for side in range(2):
                z_copy(c, stage - 1, side).wait_recv()
                rows = pl.ds(base_row(c, 0) + quarter_row(side, True), quarter)
                total = part[rows, :] + (z1, z2)[stage - 1][c, side]
                if stage == 1:
                    part[rows, :] = total
                    z_copy(c, 1, side).start()
                else:
                    state[rows, :] = total.astype(bf16)
                    for to in range(3):
                        state_copy(c, side, to).start()

    def mass_copy(seq, d):
        return pltpu.make_async_remote_copy(
            src_ref=mass.at[pl.ds(seq * HEADS, HEADS)], dst_ref=mass_in.at[seq, d],
            send_sem=mass_send.at[seq, d], recv_sem=mass_recv.at[seq, d],
            device_id=(o, lax.rem(s + d, 8)), device_id_type=MESH,
        )

    def take_mass(seq):
        for d in range(1, 8):
            mass_copy(seq, d).wait()
        rows = pl.ds(seq * HEADS, HEADS)
        total = mass[rows, :]
        for d in range(1, 8):
            total = total + mass_in[seq, d]
        mass[rows, :] = total

    def factors(seq, group):
        def one(i):
            h = group * 8 + i
            rows = pl.ds(h * PITCH, T)
            query = fa[rows, :].astype(bf16)
            q_head[seq * HEADS + h] = query
            m = mass[pl.ds(seq * HEADS + h, 1), :]
            bottom = jnp.sum(query.astype(f32) * m, axis=1, keepdims=True) + 0.001 * COUNT
            factor[seq, rows, :] = COUNT**0.5 / (bottom * factor[seq, rows, :])

        in_steps(8, one)

    def read(seq, group):
        def one(i):
            h = seq * HEADS + group * 8 + i
            block = state[pl.ds(pl.multiple_of(h * D, D), D), :]
            top = jnp.dot(q_head[h], block, preferred_element_type=f32)
            rows = pl.ds((group * 8 + i) * PITCH, T)
            q_head[h] = (top * factor[seq, rows, :]).astype(bf16)

        in_steps(8, one)

    def mixed_copy(seq, i):
        return pltpu.make_async_copy(
            q_head.at[seq * HEADS + shard(*GROUPS[1][i])], mixed_out.at[seq, i], mixed_sem.at[seq, i]
        )

    def sum_copy(seq, slab):
        return pltpu.make_async_copy(
            (fa, fb)[seq].at[pl.ds(slab * PITCH, T)], sum_out.at[seq, slab], sum_sem.at[seq, slab]
        )

    def project(seq, low, high):
        total = (fa, fb)[seq]
        names = [shard(da, db) for da, db in GROUPS[0]]

        def tile_of(tile, carry):
            left = jnp.concatenate([q_head[seq * HEADS + name] for name in names], axis=1)
            columns = pl.ds(pl.multiple_of(tile * 2 * D, 2 * D), 2 * D)
            right = jnp.concatenate(
                [w_buf[name, :, :, :, columns].reshape(D, 2 * D) for name in names], axis=0
            )
            result = jnp.dot(left, right, preferred_element_type=f32)
            for j in range(2):
                slab = 2 * tile + j
                total[pl.ds(slab * PITCH, T), :] = result[:, j * D : (j + 1) * D]
                sum_copy(seq, slab).start()
            return carry

        lax.fori_loop(low, high, tile_of, 0)

    loaded = set()

    def need(i, seq, pieces):
        for piece in pieces:
            if (i, seq, piece) not in loaded:
                loaded.add((i, seq, piece))
                load(i, seq, piece).wait()

    steps = T // TC // 2
    per = PIECES // 2
    gathered = set()

    def from_other_core(group):
        for da, db, h in ORDER:
            place = (db, da)
            if place in GROUPS[group] and (da, db, h) not in gathered:
                gathered.add((da, db, h))
                arrival(w_buf.at[shard(*place), 1 - core, h], wp_sem.at[da, db, h])
                if group == 1:
                    w_store(GROUPS[1].index(place), 1 - core, h, 1).start()

    for token in make_plan():
        kind, args = token[0], token[1:]
        if kind in ("key", "query", "gate"):
            seq, half = args
            source = {"key": 0, "query": 2, "gate": 3}[kind]
            need(source, seq, range(half * per, (half + 1) * per))
            spread(
                natural[source], factor.at[seq] if kind == "gate" else fa, seq,
                (lambda x: 1.0 + jnp.exp(-x)) if kind == "gate" else feature,
                half * steps, (half + 1) * steps,
            )
        elif kind == "value":
            need(1, args[0], range(PIECES))
            spread(v_nat, fb, args[0], lambda x: x, 0, T // TC)
        elif kind == "heads":
            seq, group, side = args
            heads(seq, (mine if side else theirs) + 4 * group)
            if side == 0:
                core_copy(2 * seq + group).start()
        elif kind == "mass":
            for d in range(1, 8):
                mass_copy(args[0], d).start()
        elif kind == "take":
            take_mass(*args)
        elif kind == "factor":
            factors(*args)
        elif kind == "sum":
            reduce(*args)
        elif kind == "weight":
            w_arrive(*ORDER[args[0]])
        elif kind == "last":
            take_state(*args)
        elif kind == "read":
            read(*args)
            if args[1] == 1:
                for i in range(LATE):
                    mixed_copy(args[0], i).start()
        else:
            seq, half = args
            from_other_core(0)
            project(seq, 4 * half, 4 * half + 4)
    from_other_core(1)

    for item in sent:
        w_copy(*item).wait_send()
    for c in range(CHUNKS):
        core_copy(c).wait_send()
        for side in range(2):
            for stage in range(2):
                z_copy(c, stage, side).wait_send()
            for to in range(3):
                state_copy(c, side, to).wait_send()
    for seq in range(SEQS):
        for slab in range(HEADS):
            sum_copy(seq, slab).wait()
        for i in range(LATE):
            mixed_copy(seq, i).wait()
    for i in range(LATE):
        for h in range(2):
            w_store(i, core, h, 0).wait()
            w_store(i, 1 - core, h, 1).wait()


def finish(sums, mixed, weight, out, sum_buf, mixed_buf, w_buf, staged, sum_sem, mixed_sem, w_sem, out_sem):
    def take_w(i):
        return pltpu.make_async_copy(weight.at[i], w_buf.at[i], w_sem.at[i])

    def take_mixed(seq):
        return pltpu.make_async_copy(mixed.at[seq], mixed_buf.at[seq], mixed_sem.at[seq])

    def take_sum(seq, slab):
        return pltpu.make_async_copy(sums.at[seq, slab], sum_buf.at[seq, slab], sum_sem.at[seq, slab])

    def put(seq, slab):
        columns = pl.ds(pl.multiple_of(slab * D, D), D)
        return pltpu.make_async_copy(staged.at[seq, slab], out.at[seq, :, columns], out_sem.at[seq, slab])

    for i in range(LATE):
        take_w(i).start()

    def start(seq, carry):
        take_mixed(seq).start()
        lax.fori_loop(0, HEADS, lambda slab, c: (take_sum(seq, slab).start(), c)[1], 0)
        return carry

    lax.fori_loop(0, SEQS, start, 0)
    for i in range(LATE):
        take_w(i).wait()

    def one(step, carry):
        seq, tile = lax.div(step, HEADS // 2), lax.rem(step, HEADS // 2)

        @pl.when(tile == 0)
        def _():
            take_mixed(seq).wait()

        left = jnp.concatenate([mixed_buf[seq, i] for i in range(LATE)], axis=1)
        columns = pl.ds(pl.multiple_of(tile * 2 * D, 2 * D), 2 * D)
        right = w_buf[:, :, :, :, columns].reshape(LATE * D, 2 * D)
        result = jnp.dot(left, right, preferred_element_type=f32)
        for j in range(2):
            slab = 2 * tile + j
            take_sum(seq, slab).wait()
            staged[seq, slab] = (sum_buf[seq, slab] + result[:, j * D : (j + 1) * D]).astype(bf16)
            put(seq, slab).start()
        return carry

    lax.fori_loop(0, SEQS * HEADS // 2, one, 0)

    def drain(step, carry):
        put(lax.div(step, HEADS), lax.rem(step, HEADS)).wait()
        return carry

    lax.fori_loop(0, SEQS * HEADS, drain, 0)


def body(queries_in, keys_in, values_in, gate_rows, out_weight):
    any_space = pl.BlockSpec(memory_space=pl.ANY)
    natural = pltpu.VMEM((SEQS, T, HEADS, D), bf16)
    wide = pltpu.VMEM((HEADS * PITCH, D), f32)
    dma = pltpu.SemaphoreType.DMA
    shapes = (
        ((SEQS, HEADS, T, D), f32),
        ((SEQS, LATE, T, D), bf16),
        ((LATE, 2, 2, ROWS, WIDTH), bf16),
    )
    late = pl.pallas_call(
        attention,
        out_shape=tuple(jax.ShapeDtypeStruct(*shape) for shape in shapes),
        in_specs=[any_space] * 5,
        out_specs=(any_space,) * 3,
        scratch_shapes=[
            natural, natural, natural, natural,
            wide, wide, pltpu.VMEM((SEQS, HEADS * PITCH, D), f32),
            pltpu.VMEM((SEQS * HEADS, T, D), bf16),
            pltpu.VMEM((SEQS * HEADS * D, D), f32),
            pltpu.VMEM((SEQS * HEADS, D), f32),
            pltpu.VMEM((SEQS, 8, HEADS, D), f32),
            pltpu.VMEM((CHUNKS, CROWS, D), f32),
            pltpu.VMEM((CHUNKS, 2, CROWS // 4, D), f32),
            pltpu.VMEM((CHUNKS, 2, CROWS // 4, D), f32),
            pltpu.VMEM((SEQS * HEADS * D, D), bf16),
            pltpu.VMEM((16, 2, 2, ROWS, WIDTH), bf16),
            dma((4, SEQS, PIECES)), dma, dma((SEQS, HEADS)), dma((SEQS, LATE)), dma((LATE, 2, 2)),
            dma((CHUNKS,)), dma((CHUNKS,)), dma((CHUNKS, 2, 2)), dma((CHUNKS, 2, 2)),
            dma((CHUNKS, 2, 3)), dma((CHUNKS, 2, 3)), dma((SEQS, 8)), dma((SEQS, 8)),
            dma((5, 4, 4, 2)), dma((4, 4, 2)), dma((4, 4, 2)),
        ],
        compiler_params=pltpu.CompilerParams(
            collective_id=0, has_side_effects=True, vmem_limit_bytes=63 * 1024 * 1024
        ),
        name="attention",
    )(queries_in, keys_in, values_in, gate_rows, out_weight.reshape(2, 2, ROWS, WIDTH))
    return pl.pallas_call(
        finish,
        out_shape=jax.ShapeDtypeStruct((SEQS, T, WIDTH), bf16),
        in_specs=[any_space] * 3,
        out_specs=any_space,
        scratch_shapes=[pltpu.VMEM(*shape) for shape in shapes] + [
            pltpu.VMEM((SEQS, HEADS, T, D), bf16),
            dma((SEQS, HEADS)), dma((SEQS,)), dma((LATE,)), dma((SEQS, HEADS)),
        ],
        compiler_params=pltpu.CompilerParams(vmem_limit_bytes=63 * 1024 * 1024),
        name="finish",
    )(*late)


def solution(mesh):
    rows = P("outer", "span", None, None)
    return jax.shard_map(
        body, mesh=mesh, in_specs=(rows, rows, rows, rows, P("outer", None)),
        out_specs=P("outer", "span", None), check_vma=False,
    )
```

```python
import functools
import jax
import jax.numpy as jnp
from jax import lax
from jax.experimental import pallas as pl
from jax.experimental.pallas import tpu as pltpu
from jax.sharding import PartitionSpec as P

f32 = jnp.float32
bf16 = jnp.bfloat16
MESH = pl.DeviceIdType.MESH

SEQS = 2
T = 512
HEADS = 16
D = 128
WIDTH = HEADS * D
COUNT = 4096
PITCH = T + 4
TC = 64
HG = 4
PIECES = 4
ROWS = 32
BLOCKS = 8
CHUNKS = 4
CROWS = 4 * D

ORDER = (
    (3, 0, 0), (1, 0, 1), (0, 3, 0), (0, 1, 1), (3, 0, 1), (1, 0, 0), (0, 3, 1), (0, 1, 0),
    (2, 0, 0), (2, 0, 1), (3, 3, 0), (3, 1, 0), (1, 1, 1), (1, 3, 1), (0, 2, 0), (0, 2, 1),
    (3, 1, 1), (3, 3, 1), (1, 3, 0), (1, 1, 0), (2, 3, 0), (2, 1, 0), (2, 1, 1), (2, 3, 1),
    (3, 2, 0), (3, 2, 1), (1, 2, 0), (1, 2, 1), (2, 2, 0), (2, 2, 1),
)
ARRIVE = (
    5.8, 5.8, 5.8, 5.8, 8.6, 8.6, 8.6, 8.6, 11.6, 11.6, 11.6, 11.6, 13.0, 13.0, 14.4, 14.4,
    15.8, 15.8, 17.2, 17.2, 18.7, 18.7, 20.1, 20.1, 21.5, 22.9, 22.9, 22.9, 24.3, 24.5,
)
GROUPS = (
    ((0, 0), (3, 0), (1, 0), (0, 3), (0, 1), (2, 0), (0, 2), (3, 3), (3, 1), (1, 3)),
    ((1, 1), (2, 3), (3, 2), (2, 1), (1, 2), (2, 2)),
)


def make_plan():
    begin, weights_at, wire, hop = 2.5, 2.4, 1.4, 3.4
    units = []
    for seq in range(SEQS):
        for half in range(2):
            units.append((("key", seq, half), 0.47, ()))
        units.append((("value", seq), 0.35, ()))
        for side in range(2):
            for group in range(2):
                units.append((("heads", seq, group, side), 0.3, ()))
        units.append((("mass", seq), 0.05, ()))
    for seq in range(SEQS):
        for half in range(2):
            units.append((("query", seq, half), 0.47, ()))
        for half in range(2):
            units.append((("gate", seq, half), 0.4, ()))
        units.append((("take", seq), 0.15, ()))
        for group in range(4):
            units.append((("factor", seq, group), 0.35, ()))
    first_work = len(units)
    for seq in range(SEQS):
        for group in range(2):
            c = 2 * seq + group
            units.append((("last", c), 0.02, (("sum", 4, c),)))
        for group in range(4):
            units.append((("read", seq, group), 0.3, (("last", 2 * seq), ("last", 2 * seq + 1))))
    for half in range(2):
        for seq in range(SEQS):
            for quarter in range(4):
                before = (("read", seq, 3),) if half == 0 else (("project", 0, seq, 3),)
                units.append((("project", half, seq, quarter), (0.75, 0.48)[half], before + (("here", half),)))

    ready = {("weight", i): weights_at + at for i, at in enumerate(ARRIVE)}
    plan, done, clock, link = [], set(), begin, 0.0
    left = list(range(len(units)))
    while left or ready:
        due = [e for e in ready if ready[e] <= clock]
        able = [i for i in left if all(n in done for n in units[i][2])]
        if left and left[0] < first_work:
            able = left[:1]
        if due:
            token = min(due, key=lambda e: (ready[e], e))
        elif able:
            left.remove(able[0])
            token, cost, _ = units[able[0]]
            clock += cost
            if token[0] == "heads" and token[3] == 0:
                ready["sum", 0, 2 * token[1] + token[2]] = clock + 1.6
        else:
            token = min(ready, key=lambda e: (ready[e], e))
            clock = ready[token]
        if token in ready:
            del ready[token]
            clock += (0.25, 0.15, 0.15, 0.02, 0.0)[token[1]] if token[0] == "sum" else 0.05
            if token in (("weight", 18), ("weight", 29)):
                ready["here", int(token[1] == 29)] = clock + 1.6
            if token[0] == "sum" and token[1] < 3:
                link = max(link, clock) + wire / (1 if token[1] < 2 else 2)
                ready["sum", token[1] + 1, token[2]] = link + hop
            elif token[0] == "sum" and token[1] == 3:
                ready["sum", 4, token[2]] = clock + 1.4
        done.add(token)
        if token[:2] != ("sum", 4) and token[0] != "here":
            plan.append(token)
    return plan


def feature(x):
    return jnp.maximum(x, 0.0) + jnp.exp(jnp.minimum(x, 0.0))


def spread(src, dst, seq, fn, low, high):
    def step(i, carry):
        start = i * TC
        values = fn(src[seq, pl.ds(start, TC)].astype(f32))
        for t in range(TC):
            for half in range(2):
                dst[pl.ds(start + t + 8 * half * PITCH, 8, stride=PITCH), :] = values[
                    t, 8 * half : 8 * half + 8, :
                ]
        return carry

    lax.fori_loop(low, high, step, 0)


def attention(
    q_in, k_in, v_in, g_in, w_in,
    out,
    q_nat, k_nat, v_nat, g_nat,
    fa, fb, factor, q_head, part, mass, mass_in,
    core_in, z1, z2, state, staged, w_buf,
    load_sem, w_load_sem, out_sem,
    core_send, core_recv, z_send, z_recv, st_send, st_recv, mass_send, mass_recv,
    ws_sem, wr_sem, wp_sem,
):
    o = lax.axis_index("outer")
    s = lax.axis_index("span")
    core = lax.rem(s, 2)
    z = lax.div(s, 2)
    other = s + 1 - 2 * core
    first = s + 2 * (1 - 2 * lax.rem(z, 2))
    second = 2 * (3 - z) + core
    upper = lax.div(z, 2)
    gray = lax.rem(z + upper, 2)
    sa = 1 + 3 * core
    sb = 4 - 3 * core
    a = lax.rem(lax.div(o, sa), 4)
    b = lax.rem(lax.div(o, sb), 4)

    def shard(da, db):
        return lax.rem(a + da, 4) * sa + lax.rem(b + db, 4) * sb

    arrays = (k_in, v_in, q_in, g_in)
    natural = (k_nat, v_nat, q_nat, g_nat)
    step = T // PIECES

    def load(i, seq, piece):
        rows = pl.ds(piece * step, step)
        return pltpu.make_async_copy(
            arrays[i].at[seq, rows], natural[i].at[seq, rows], load_sem.at[i, seq, piece]
        )

    own_w = pltpu.make_async_copy(w_in, w_buf.at[o], w_load_sem)
    own_w.start()
    for pair in ((0, 1), (2, 3)):
        for seq in range(SEQS):
            for i in pair:
                for piece in range(PIECES):
                    load(i, seq, piece).start()

    barrier = pltpu.get_barrier_semaphore()
    for da, db in ((1, 0), (3, 0), (0, 1), (0, 3)):
        pl.semaphore_signal(barrier, inc=1, device_id=(shard(da, db), s), device_id_type=MESH)
    for d in range(1, 8):
        pl.semaphore_signal(barrier, inc=1, device_id=(o, lax.rem(s + d, 8)), device_id_type=MESH)
    own_w.wait()
    pl.semaphore_wait(barrier, 11)

    kinds = {"A+": (1, 0), "A-": (3, 0), "B+": (0, 1), "B-": (0, 3)}
    sent = []

    def w_copy(kind, da, db, h):
        ref = w_buf.at[shard(da, db), core, h]
        if kind == "P":
            return pltpu.make_async_remote_copy(
                src_ref=ref, dst_ref=ref, send_sem=ws_sem.at[4, da, db, h], recv_sem=wp_sem.at[da, db, h],
                device_id=(o, other), device_id_type=MESH,
            )
        ka, kb = kinds[kind]
        return pltpu.make_async_remote_copy(
            src_ref=ref,
            dst_ref=ref,
            send_sem=ws_sem.at[list(kinds).index(kind), da, db, h],
            recv_sem=wr_sem.at[(da - ka) % 4, (db - kb) % 4, h],
            device_id=(shard(ka, kb), s),
            device_id_type=MESH,
        )

    def w_send(kind, da, db, h):
        w_copy(kind, da, db, h).start()
        sent.append((kind, da, db, h))

    def arrival(ref, sem):
        pltpu.make_async_remote_copy(
            src_ref=ref, dst_ref=ref, send_sem=ws_sem.at[0, 0, 0, 0], recv_sem=sem,
            device_id=(o, other), device_id_type=MESH,
        ).wait_recv()

    def w_arrive(da, db, h):
        arrival(w_buf.at[shard(da, db), core, h], wr_sem.at[da, db, h])
        if db == 0:
            if da == 3 and h == 0:
                w_send("A+", da, db, h)
            if da == 1 and h == 1:
                w_send("A-", da, db, h)
            w_send("B+", da, db, h)
            w_send("B-", da, db, h)
        elif db == 3 and h == 0:
            w_send("B+", da, db, h)
        elif db == 1 and h == 1:
            w_send("B-", da, db, h)
        w_send("P", da, db, h)

    for names, h in ((("A+", "B+"), 0), (("A-", "B-"), 1), (("A+", "B+"), 1), (("A-", "B-"), 0)):
        for name in names:
            w_send(name, 0, 0, h)

    mine = core * 8
    theirs = 8 - mine

    def heads(seq, base):
        for j in range(HG):
            h = base + j
            key = fa[pl.ds(h * PITCH, T), :].astype(bf16)
            value = fb[pl.ds(h * PITCH, T), :].astype(bf16)
            part[pl.ds((seq * HEADS + h) * D, D), :] = lax.dot_general(
                key, value, (((0,), (0,)), ((), ())), preferred_element_type=f32
            )
            m = jnp.sum(key.astype(f32).reshape(T // 8, 8, D), axis=0)
            mass[pl.ds(seq * HEADS + h, 1), :] = jnp.sum(m, axis=0, keepdims=True)

    def base_row(c, side):
        return ((c // 2) * HEADS + (theirs if side else mine) + 4 * (c % 2)) * D

    def core_copy(c):
        return pltpu.make_async_remote_copy(
            src_ref=part.at[pl.ds(base_row(c, 1), CROWS)], dst_ref=core_in.at[c],
            send_sem=core_send.at[c], recv_sem=core_recv.at[c],
            device_id=(o, other), device_id_type=MESH,
        )

    half_rows, quarter = CROWS // 2, CROWS // 4
    bits = (gray, upper)
    peers = ((first, second), (second, first))

    def quarter_row(side, keep):
        bit = bits[side] if keep else 1 - bits[side]
        return side * half_rows + bit * quarter

    def z_copy(c, stage, side):
        src = part.at[pl.ds(base_row(c, 0) + quarter_row(side, stage == 1), quarter)]
        return pltpu.make_async_remote_copy(
            src_ref=src, dst_ref=(z1, z2)[stage].at[c, side],
            send_sem=z_send.at[c, stage, side], recv_sem=z_recv.at[c, stage, side],
            device_id=(o, peers[side][stage]), device_id_type=MESH,
        )

    def quarter_copy(c, side):
        rows = pl.ds(base_row(c, 0) + quarter_row(side, True), quarter)
        return pltpu.make_async_remote_copy(
            src_ref=state.at[rows], dst_ref=state.at[rows],
            send_sem=z_send.at[c, 2, side], recv_sem=z_recv.at[c, 2, side],
            device_id=(o, peers[side][0]), device_id_type=MESH,
        )

    def state_copy(c):
        rows = pl.ds(base_row(c, 0), CROWS)
        return pltpu.make_async_remote_copy(
            src_ref=state.at[rows], dst_ref=state.at[rows],
            send_sem=st_send.at[c], recv_sem=st_recv.at[c],
            device_id=(o, other), device_id_type=MESH,
        )

    def take_state(c):
        arrival(state.at[pl.ds(base_row(c, 1), CROWS)], st_recv.at[c])

    def reduce(stage, c):
        if stage == 0:
            core_copy(c).wait_recv()
            rows = pl.ds(base_row(c, 0), CROWS)
            part[rows, :] = part[rows, :] + core_in[c]
            for side in range(2):
                z_copy(c, 0, side).start()
        elif stage == 3:
            for side in range(2):
                rows = pl.ds(base_row(c, 0) + quarter_row(side, False), quarter)
                arrival(state.at[rows], z_recv.at[c, 2, side])
            state_copy(c).start()
        else:
            for side in range(2):
                z_copy(c, stage - 1, side).wait_recv()
                rows = pl.ds(base_row(c, 0) + quarter_row(side, True), quarter)
                total = part[rows, :] + (z1, z2)[stage - 1][c, side]
                if stage == 1:
                    part[rows, :] = total
                    z_copy(c, 1, side).start()
                else:
                    state[rows, :] = total.astype(bf16)
                    quarter_copy(c, side).start()

    def mass_copy(seq, d):
        return pltpu.make_async_remote_copy(
            src_ref=mass.at[pl.ds(seq * HEADS, HEADS)], dst_ref=mass_in.at[seq, d],
            send_sem=mass_send.at[seq, d], recv_sem=mass_recv.at[seq, d],
            device_id=(o, lax.rem(s + d, 8)), device_id_type=MESH,
        )

    def take_mass(seq):
        for d in range(1, 8):
            mass_copy(seq, d).wait()
        rows = pl.ds(seq * HEADS, HEADS)
        total = mass[rows, :]
        for d in range(1, 8):
            total = total + mass_in[seq, d]
        mass[rows, :] = total

    def factors(seq, group):
        for j in range(HG):
            h = group * HG + j
            rows = pl.ds(h * PITCH, T)
            query = fa[rows, :].astype(bf16)
            q_head[seq * HEADS + h] = query
            m = mass[pl.ds(seq * HEADS + h, 1), :]
            bottom = jnp.sum(query.astype(f32) * m, axis=1, keepdims=True) + 0.001 * COUNT
            factor[seq, rows, :] = COUNT**0.5 / (bottom * factor[seq, rows, :])

    def read(seq, group):
        for j in range(HG):
            h = seq * HEADS + group * HG + j
            top = jnp.dot(q_head[h], state[h * D : (h + 1) * D, :], preferred_element_type=f32)
            rows = pl.ds((group * HG + j) * PITCH, T)
            q_head[h] = (top * factor[seq, rows, :]).astype(bf16)

    def out_copy(seq, slab):
        columns = pl.ds(pl.multiple_of(slab * D, D), D)
        return pltpu.make_async_copy(
            staged.at[seq, slab], out.at[seq, :, columns], out_sem.at[seq, slab]
        )

    def project(half, seq, tiles):
        total = (fa, fb)[seq]
        names = [shard(da, db) for da, db in GROUPS[half]]
        left = jnp.concatenate([q_head[seq * HEADS + name] for name in names], axis=1)
        for tile in tiles:
            columns = slice(tile * 2 * D, (tile + 1) * 2 * D)
            right = jnp.concatenate(
                [w_buf[name, :, :, :, columns].reshape(D, 2 * D) for name in names], axis=0
            )
            result = jnp.dot(left, right, preferred_element_type=f32)
            for j in range(2):
                slab = 2 * tile + j
                piece = result[:, j * D : (j + 1) * D]
                rows = pl.ds(slab * PITCH, T)
                if half == 0:
                    total[rows, :] = piece
                else:
                    staged[seq, slab] = (total[rows, :] + piece).astype(bf16)
                    out_copy(seq, slab).start()

    loaded = set()

    def need(i, seq, pieces):
        for piece in pieces:
            if (i, seq, piece) not in loaded:
                loaded.add((i, seq, piece))
                load(i, seq, piece).wait()

    steps = T // TC // 2
    per = PIECES // 2
    gathered = set()
    for token in make_plan():
        kind, args = token[0], token[1:]
        if kind in ("key", "query", "gate"):
            seq, half = args
            source = {"key": 0, "query": 2, "gate": 3}[kind]
            need(source, seq, range(half * per, (half + 1) * per))
            spread(
                natural[source], factor.at[seq] if kind == "gate" else fa, seq,
                (lambda x: 1.0 + jnp.exp(-x)) if kind == "gate" else feature,
                half * steps, (half + 1) * steps,
            )
        elif kind == "value":
            need(1, args[0], range(PIECES))
            spread(v_nat, fb, args[0], lambda x: x, 0, T // TC)
        elif kind == "heads":
            seq, group, side = args
            heads(seq, (mine if side else theirs) + 4 * group)
            if side == 0:
                core_copy(2 * seq + group).start()
        elif kind == "mass":
            for d in range(1, 8):
                mass_copy(args[0], d).start()
        elif kind == "take":
            take_mass(*args)
        elif kind == "factor":
            factors(*args)
        elif kind == "sum":
            reduce(*args)
        elif kind == "weight":
            w_arrive(*ORDER[args[0]])
        elif kind == "last":
            take_state(*args)
        elif kind == "read":
            read(*args)
        else:
            half, seq, quarter_of = args
            for da, db, h in ORDER:
                if (db, da) in GROUPS[half] and (da, db, h) not in gathered:
                    gathered.add((da, db, h))
                    arrival(w_buf.at[shard(db, da), 1 - core, h], wp_sem.at[da, db, h])
            project(half, seq, range(quarter_of * 2, quarter_of * 2 + 2))

    for item in sent:
        w_copy(*item).wait_send()
    for c in range(CHUNKS):
        core_copy(c).wait_send()
        for side in range(2):
            for stage in range(2):
                z_copy(c, stage, side).wait_send()
            quarter_copy(c, side).wait_send()
        state_copy(c).wait_send()
    for seq in range(SEQS):
        for slab in range(HEADS):
            out_copy(seq, slab).wait()


def hand_over(src, dst, buffer, in_sem, out_sem):
    blocks = [(seq, i) for seq in range(SEQS) for i in range(BLOCKS)]
    rows = [pl.ds(i * (T // BLOCKS), T // BLOCKS) for i in range(BLOCKS)]

    def fetch(seq, i):
        return pltpu.make_async_copy(src.at[seq, rows[i]], buffer.at[seq, rows[i]], in_sem.at[seq, i])

    def put(seq, i):
        return pltpu.make_async_copy(buffer.at[seq, rows[i]], dst.at[seq, rows[i]], out_sem.at[seq, i])

    for block in blocks:
        fetch(*block).start()
    for block in blocks:
        fetch(*block).wait()
        put(*block).start()
    for block in blocks:
        put(*block).wait()


def body(queries_in, keys_in, values_in, gate_rows, out_weight):
    any_space = pl.BlockSpec(memory_space=pl.ANY)
    natural = pltpu.VMEM((SEQS, T, HEADS, D), bf16)
    wide = pltpu.VMEM((HEADS * PITCH, D), f32)
    dma = pltpu.SemaphoreType.DMA
    result = pl.pallas_call(
        attention,
        out_shape=jax.ShapeDtypeStruct((SEQS, T, WIDTH), bf16),
        in_specs=[any_space] * 5,
        out_specs=any_space,
        scratch_shapes=[
            natural, natural, natural, natural,
            wide, wide, pltpu.VMEM((SEQS, HEADS * PITCH, D), f32),
            pltpu.VMEM((SEQS * HEADS, T, D), bf16),
            pltpu.VMEM((SEQS * HEADS * D, D), f32),
            pltpu.VMEM((SEQS * HEADS, D), f32),
            pltpu.VMEM((SEQS, 8, HEADS, D), f32),
            pltpu.VMEM((CHUNKS, CROWS, D), f32),
            pltpu.VMEM((CHUNKS, 2, CROWS // 4, D), f32),
            pltpu.VMEM((CHUNKS, 2, CROWS // 4, D), f32),
            pltpu.VMEM((SEQS * HEADS * D, D), bf16),
            pltpu.VMEM((SEQS, HEADS, T, D), bf16),
            pltpu.VMEM((16, 2, 2, ROWS, WIDTH), bf16),
            dma((4, SEQS, PIECES)), dma, dma((SEQS, HEADS)),
            dma((CHUNKS,)), dma((CHUNKS,)), dma((CHUNKS, 3, 2)), dma((CHUNKS, 3, 2)),
            dma((CHUNKS,)), dma((CHUNKS,)), dma((SEQS, 8)), dma((SEQS, 8)),
            dma((5, 4, 4, 2)), dma((4, 4, 2)), dma((4, 4, 2)),
        ],
        compiler_params=pltpu.CompilerParams(
            collective_id=0, has_side_effects=True, vmem_limit_bytes=63 * 1024 * 1024
        ),
        name="attention",
    )(queries_in, keys_in, values_in, gate_rows, out_weight.reshape(2, 2, ROWS, WIDTH))
    return pl.pallas_call(
        hand_over,
        out_shape=jax.ShapeDtypeStruct((SEQS, T, WIDTH), bf16),
        in_specs=[any_space],
        out_specs=any_space,
        scratch_shapes=[pltpu.VMEM((SEQS, T, WIDTH), bf16), dma((SEQS, BLOCKS)), dma((SEQS, BLOCKS))],
        compiler_params=pltpu.CompilerParams(vmem_limit_bytes=63 * 1024 * 1024),
        name="hand_over",
    )(result)


def solution(mesh):
    rows = P("outer", "span", None, None)
    return jax.shard_map(
        body, mesh=mesh, in_specs=(rows, rows, rows, rows, P("outer", None)),
        out_specs=P("outer", "span", None), check_vma=False,
    )
```

```python
import functools
import jax
import jax.numpy as jnp
from jax import lax
from jax.experimental import pallas as pl
from jax.experimental.pallas import tpu as pltpu
from jax.sharding import PartitionSpec as P

f32 = jnp.float32
bf16 = jnp.bfloat16
MESH = pl.DeviceIdType.MESH

SEQS = 2
T = 512
HEADS = 16
D = 128
WIDTH = HEADS * D
COUNT = 4096
PITCH = T + 4
TC = 64
HG = 4
PIECES = 4
ROWS = 32
BLOCKS = 8
CHUNKS = 4
CROWS = 4 * D

ORDER = (
    (3, 0, 0), (1, 0, 1), (0, 3, 0), (0, 1, 1), (3, 0, 1), (1, 0, 0), (0, 3, 1), (0, 1, 0),
    (2, 0, 0), (2, 0, 1), (3, 3, 0), (3, 1, 0), (1, 1, 1), (1, 3, 1), (0, 2, 0), (0, 2, 1),
    (3, 1, 1), (3, 3, 1), (1, 3, 0), (1, 1, 0), (2, 3, 0), (2, 1, 0), (2, 1, 1), (2, 3, 1),
    (3, 2, 0), (3, 2, 1), (1, 2, 0), (1, 2, 1), (2, 2, 0), (2, 2, 1),
)
ARRIVE = (
    5.8, 5.8, 5.8, 5.8, 8.6, 8.6, 8.6, 8.6, 11.6, 11.6, 11.6, 11.6, 13.0, 13.0, 14.4, 14.4,
    15.8, 15.8, 17.2, 17.2, 18.7, 18.7, 20.1, 20.1, 21.5, 22.9, 22.9, 22.9, 24.3, 24.5,
)
GROUPS = (
    ((0, 0), (3, 0), (1, 0), (0, 3), (0, 1), (2, 0), (0, 2), (3, 3), (3, 1), (1, 3)),
    ((1, 1), (2, 3), (3, 2), (2, 1), (1, 2), (2, 2)),
)


def make_plan():
    begin, weights_at, wire, hop = 1.5, 1.5, 1.4, 3.4
    units = []
    for seq in range(SEQS):
        for half in range(2):
            units.append((("key", seq, half), 0.47, ()))
        units.append((("value", seq), 0.35, ()))
        for side in range(2):
            for group in range(2):
                units.append((("heads", seq, group, side), 0.3, ()))
        units.append((("mass", seq), 0.05, ()))
    for seq in range(SEQS):
        for half in range(2):
            units.append((("query", seq, half), 0.47, ()))
        for half in range(2):
            units.append((("gate", seq, half), 0.4, ()))
        units.append((("take", seq), 0.15, ()))
        for group in range(4):
            units.append((("factor", seq, group), 0.35, ()))
    first_work = len(units)
    for seq in range(SEQS):
        for group in range(2):
            c = 2 * seq + group
            units.append((("last", c), 0.02, (("sum", 4, c),)))
            for four in (group, group + 2):
                units.append((("read", seq, four), 0.3, (("last", c),)))
    for half in range(2):
        for seq in range(SEQS):
            for quarter in range(4):
                before = tuple(("read", seq, four) for four in range(4)) if half == 0 else (("project", 0, seq, 3),)
                units.append((("project", half, seq, quarter), (0.75, 0.48)[half], before + (("here", half),)))

    ready = {("weight", i): weights_at + at for i, at in enumerate(ARRIVE)}
    plan, done, clock, link = [], set(), begin, 0.0
    left = list(range(len(units)))
    while left or ready:
        due = [e for e in ready if ready[e] <= clock]
        able = [i for i in left if all(n in done for n in units[i][2])]
        if left and left[0] < first_work:
            able = left[:1]
        if due:
            token = min(due, key=lambda e: (ready[e], e))
        elif able:
            left.remove(able[0])
            token, cost, _ = units[able[0]]
            clock += cost
            if token[0] == "heads" and token[3] == 0:
                ready["sum", 0, 2 * token[1] + token[2]] = clock + 1.6
        else:
            token = min(ready, key=lambda e: (ready[e], e))
            clock = ready[token]
        if token in ready:
            del ready[token]
            clock += (0.25, 0.15, 0.15, 0.02, 0.0)[token[1]] if token[0] == "sum" else 0.05
            if token in (("weight", 18), ("weight", 29)):
                ready["here", int(token[1] == 29)] = clock + 1.6
            if token[0] == "sum" and token[1] < 3:
                link = max(link, clock) + wire / (1 if token[1] < 2 else 2)
                ready["sum", token[1] + 1, token[2]] = link + hop
            elif token[0] == "sum" and token[1] == 3:
                ready["sum", 4, token[2]] = clock + 1.4
        done.add(token)
        if token[:2] != ("sum", 4) and token[0] != "here":
            plan.append(token)
    return plan


def feature(x):
    return jnp.maximum(x, 0.0) + jnp.exp(jnp.minimum(x, 0.0))


def spread(src, dst, seq, fn, low, high):
    def step(i, carry):
        start = i * TC
        values = fn(src[seq, pl.ds(start, TC)].astype(f32))
        for t in range(TC):
            for half in range(2):
                dst[pl.ds(start + t + 8 * half * PITCH, 8, stride=PITCH), :] = values[
                    t, 8 * half : 8 * half + 8, :
                ]
        return carry

    lax.fori_loop(low, high, step, 0)


def attention(
    q_in, k_in, v_in, g_in, w_in,
    out,
    q_nat, k_nat, v_nat, g_nat,
    fa, fb, factor, q_head, part, mass, mass_in,
    core_in, z1, z2, state, staged, w_buf,
    load_sem, w_load_sem, out_sem,
    core_send, core_recv, z_send, z_recv, st_send, st_recv, mass_send, mass_recv,
    ws_sem, wr_sem, wp_sem,
):
    o = lax.axis_index("outer")
    s = lax.axis_index("span")
    core = lax.rem(s, 2)
    z = lax.div(s, 2)
    other = s + 1 - 2 * core
    first = s + 2 * (1 - 2 * lax.rem(z, 2))
    second = 2 * (3 - z) + core
    upper = lax.div(z, 2)
    gray = lax.rem(z + upper, 2)
    sa = 1 + 3 * core
    sb = 4 - 3 * core
    a = lax.rem(lax.div(o, sa), 4)
    b = lax.rem(lax.div(o, sb), 4)

    def shard(da, db):
        return lax.rem(a + da, 4) * sa + lax.rem(b + db, 4) * sb

    arrays = (k_in, v_in, q_in, g_in)
    natural = (k_nat, v_nat, q_nat, g_nat)
    step = T // PIECES

    def load(i, seq, piece):
        rows = pl.ds(piece * step, step)
        return pltpu.make_async_copy(
            arrays[i].at[seq, rows], natural[i].at[seq, rows], load_sem.at[i, seq, piece]
        )

    own_w = pltpu.make_async_copy(w_in, w_buf.at[o], w_load_sem)
    own_w.start()
    for pair in ((0, 1), (2, 3)):
        for seq in range(SEQS):
            for i in pair:
                for piece in range(PIECES):
                    load(i, seq, piece).start()

    barrier = pltpu.get_barrier_semaphore()
    for da, db in ((1, 0), (3, 0), (0, 1), (0, 3)):
        pl.semaphore_signal(barrier, inc=1, device_id=(shard(da, db), s), device_id_type=MESH)
    for d in range(1, 8):
        pl.semaphore_signal(barrier, inc=1, device_id=(o, lax.rem(s + d, 8)), device_id_type=MESH)
    own_w.wait()
    pl.semaphore_wait(barrier, 11)

    kinds = {"A+": (1, 0), "A-": (3, 0), "B+": (0, 1), "B-": (0, 3)}
    sent = []

    def w_copy(kind, da, db, h):
        ref = w_buf.at[shard(da, db), core, h]
        if kind == "P":
            return pltpu.make_async_remote_copy(
                src_ref=ref, dst_ref=ref, send_sem=ws_sem.at[4, da, db, h], recv_sem=wp_sem.at[da, db, h],
                device_id=(o, other), device_id_type=MESH,
            )
        ka, kb = kinds[kind]
        return pltpu.make_async_remote_copy(
            src_ref=ref,
            dst_ref=ref,
            send_sem=ws_sem.at[list(kinds).index(kind), da, db, h],
            recv_sem=wr_sem.at[(da - ka) % 4, (db - kb) % 4, h],
            device_id=(shard(ka, kb), s),
            device_id_type=MESH,
        )

    def w_send(kind, da, db, h):
        w_copy(kind, da, db, h).start()
        sent.append((kind, da, db, h))

    def arrival(ref, sem):
        pltpu.make_async_remote_copy(
            src_ref=ref, dst_ref=ref, send_sem=ws_sem.at[0, 0, 0, 0], recv_sem=sem,
            device_id=(o, other), device_id_type=MESH,
        ).wait_recv()

    def w_arrive(da, db, h):
        arrival(w_buf.at[shard(da, db), core, h], wr_sem.at[da, db, h])
        if db == 0:
            if da == 3 and h == 0:
                w_send("A+", da, db, h)
            if da == 1 and h == 1:
                w_send("A-", da, db, h)
            w_send("B+", da, db, h)
            w_send("B-", da, db, h)
        elif db == 3 and h == 0:
            w_send("B+", da, db, h)
        elif db == 1 and h == 1:
            w_send("B-", da, db, h)
        w_send("P", da, db, h)

    for names, h in ((("A+", "B+"), 0), (("A-", "B-"), 1), (("A+", "B+"), 1), (("A-", "B-"), 0)):
        for name in names:
            w_send(name, 0, 0, h)

    mine = core * 8
    theirs = 8 - mine

    def heads(seq, base):
        for j in range(HG):
            h = base + j
            key = fa[pl.ds(h * PITCH, T), :].astype(bf16)
            value = fb[pl.ds(h * PITCH, T), :].astype(bf16)
            part[pl.ds((seq * HEADS + h) * D, D), :] = lax.dot_general(
                key, value, (((0,), (0,)), ((), ())), preferred_element_type=f32
            )
            m = jnp.sum(key.astype(f32).reshape(T // 8, 8, D), axis=0)
            mass[pl.ds(seq * HEADS + h, 1), :] = jnp.sum(m, axis=0, keepdims=True)

    def base_row(c, side):
        return ((c // 2) * HEADS + (theirs if side else mine) + 4 * (c % 2)) * D

    def core_copy(c):
        return pltpu.make_async_remote_copy(
            src_ref=part.at[pl.ds(base_row(c, 1), CROWS)], dst_ref=core_in.at[c],
            send_sem=core_send.at[c], recv_sem=core_recv.at[c],
            device_id=(o, other), device_id_type=MESH,
        )

    half_rows, quarter = CROWS // 2, CROWS // 4
    bits = (gray, upper)
    peers = ((first, second), (second, first))

    def quarter_row(side, keep):
        bit = bits[side] if keep else 1 - bits[side]
        return side * half_rows + bit * quarter

    def z_copy(c, stage, side):
        src = part.at[pl.ds(base_row(c, 0) + quarter_row(side, stage == 1), quarter)]
        return pltpu.make_async_remote_copy(
            src_ref=src, dst_ref=(z1, z2)[stage].at[c, side],
            send_sem=z_send.at[c, stage, side], recv_sem=z_recv.at[c, stage, side],
            device_id=(o, peers[side][stage]), device_id_type=MESH,
        )

    def quarter_copy(c, side):
        rows = pl.ds(base_row(c, 0) + quarter_row(side, True), quarter)
        return pltpu.make_async_remote_copy(
            src_ref=state.at[rows], dst_ref=state.at[rows],
            send_sem=z_send.at[c, 2, side], recv_sem=z_recv.at[c, 2, side],
            device_id=(o, peers[side][0]), device_id_type=MESH,
        )

    def state_copy(c):
        rows = pl.ds(base_row(c, 0), CROWS)
        return pltpu.make_async_remote_copy(
            src_ref=state.at[rows], dst_ref=state.at[rows],
            send_sem=st_send.at[c], recv_sem=st_recv.at[c],
            device_id=(o, other), device_id_type=MESH,
        )

    def take_state(c):
        arrival(state.at[pl.ds(base_row(c, 1), CROWS)], st_recv.at[c])

    def reduce(stage, c):
        if stage == 0:
            core_copy(c).wait_recv()
            rows = pl.ds(base_row(c, 0), CROWS)
            part[rows, :] = part[rows, :] + core_in[c]
            for side in range(2):
                z_copy(c, 0, side).start()
        elif stage == 3:
            for side in range(2):
                rows = pl.ds(base_row(c, 0) + quarter_row(side, False), quarter)
                arrival(state.at[rows], z_recv.at[c, 2, side])
            state_copy(c).start()
        else:
            for side in range(2):
                z_copy(c, stage - 1, side).wait_recv()
                rows = pl.ds(base_row(c, 0) + quarter_row(side, True), quarter)
                total = part[rows, :] + (z1, z2)[stage - 1][c, side]
                if stage == 1:
                    part[rows, :] = total
                    z_copy(c, 1, side).start()
                else:
                    state[rows, :] = total.astype(bf16)
                    quarter_copy(c, side).start()

    def mass_copy(seq, d):
        return pltpu.make_async_remote_copy(
            src_ref=mass.at[pl.ds(seq * HEADS, HEADS)], dst_ref=mass_in.at[seq, d],
            send_sem=mass_send.at[seq, d], recv_sem=mass_recv.at[seq, d],
            device_id=(o, lax.rem(s + d, 8)), device_id_type=MESH,
        )

    def take_mass(seq):
        for d in range(1, 8):
            mass_copy(seq, d).wait()
        rows = pl.ds(seq * HEADS, HEADS)
        total = mass[rows, :]
        for d in range(1, 8):
            total = total + mass_in[seq, d]
        mass[rows, :] = total

    def factors(seq, group):
        for j in range(HG):
            h = group * HG + j
            rows = pl.ds(h * PITCH, T)
            query = fa[rows, :].astype(bf16)
            q_head[seq * HEADS + h] = query
            m = mass[pl.ds(seq * HEADS + h, 1), :]
            bottom = jnp.sum(query.astype(f32) * m, axis=1, keepdims=True) + 0.001 * COUNT
            factor[seq, rows, :] = COUNT**0.5 / (bottom * factor[seq, rows, :])

    def read(seq, group):
        for j in range(HG):
            h = seq * HEADS + group * HG + j
            top = jnp.dot(q_head[h], state[h * D : (h + 1) * D, :], preferred_element_type=f32)
            rows = pl.ds((group * HG + j) * PITCH, T)
            q_head[h] = (top * factor[seq, rows, :]).astype(bf16)

    def out_copy(seq, slab):
        columns = pl.ds(pl.multiple_of(slab * D, D), D)
        return pltpu.make_async_copy(
            staged.at[seq, slab], out.at[seq, :, columns], out_sem.at[seq, slab]
        )

    def project(half, seq, tiles):
        total = (fa, fb)[seq]
        names = [shard(da, db) for da, db in GROUPS[half]]
        left = jnp.concatenate([q_head[seq * HEADS + name] for name in names], axis=1)
        for tile in tiles:
            columns = slice(tile * 2 * D, (tile + 1) * 2 * D)
            right = jnp.concatenate(
                [w_buf[name, :, :, :, columns].reshape(D, 2 * D) for name in names], axis=0
            )
            result = jnp.dot(left, right, preferred_element_type=f32)
            for j in range(2):
                slab = 2 * tile + j
                piece = result[:, j * D : (j + 1) * D]
                rows = pl.ds(slab * PITCH, T)
                if half == 0:
                    total[rows, :] = piece
                else:
                    staged[seq, slab] = (total[rows, :] + piece).astype(bf16)
                    out_copy(seq, slab).start()

    loaded = set()

    def need(i, seq, pieces):
        for piece in pieces:
            if (i, seq, piece) not in loaded:
                loaded.add((i, seq, piece))
                load(i, seq, piece).wait()

    steps = T // TC // 2
    per = PIECES // 2
    gathered = set()
    for token in make_plan():
        kind, args = token[0], token[1:]
        if kind in ("key", "query", "gate"):
            seq, half = args
            source = {"key": 0, "query": 2, "gate": 3}[kind]
            need(source, seq, range(half * per, (half + 1) * per))
            spread(
                natural[source], factor.at[seq] if kind == "gate" else fa, seq,
                (lambda x: 1.0 + jnp.exp(-x)) if kind == "gate" else feature,
                half * steps, (half + 1) * steps,
            )
        elif kind == "value":
            need(1, args[0], range(PIECES))
            spread(v_nat, fb, args[0], lambda x: x, 0, T // TC)
        elif kind == "heads":
            seq, group, side = args
            heads(seq, (mine if side else theirs) + 4 * group)
            if side == 0:
                core_copy(2 * seq + group).start()
        elif kind == "mass":
            for d in range(1, 8):
                mass_copy(args[0], d).start()
        elif kind == "take":
            take_mass(*args)
        elif kind == "factor":
            factors(*args)
        elif kind == "sum":
            reduce(*args)
        elif kind == "weight":
            w_arrive(*ORDER[args[0]])
        elif kind == "last":
            take_state(*args)
        elif kind == "read":
            read(*args)
        else:
            half, seq, quarter_of = args
            for da, db, h in ORDER:
                if (db, da) in GROUPS[half] and (da, db, h) not in gathered:
                    gathered.add((da, db, h))
                    arrival(w_buf.at[shard(db, da), 1 - core, h], wp_sem.at[da, db, h])
            project(half, seq, range(quarter_of * 2, quarter_of * 2 + 2))

    for item in sent:
        w_copy(*item).wait_send()
    for c in range(CHUNKS):
        core_copy(c).wait_send()
        for side in range(2):
            for stage in range(2):
                z_copy(c, stage, side).wait_send()
            quarter_copy(c, side).wait_send()
        state_copy(c).wait_send()
    for seq in range(SEQS):
        for slab in range(HEADS):
            out_copy(seq, slab).wait()


def hand_over(src, dst, buffer, in_sem, out_sem):
    blocks = [(seq, i) for seq in range(SEQS) for i in range(BLOCKS)]
    rows = [pl.ds(i * (T // BLOCKS), T // BLOCKS) for i in range(BLOCKS)]

    def fetch(seq, i):
        return pltpu.make_async_copy(src.at[seq, rows[i]], buffer.at[seq, rows[i]], in_sem.at[seq, i])

    def put(seq, i):
        return pltpu.make_async_copy(buffer.at[seq, rows[i]], dst.at[seq, rows[i]], out_sem.at[seq, i])

    for block in blocks:
        fetch(*block).start()
    for block in blocks:
        fetch(*block).wait()
        put(*block).start()
    for block in blocks:
        put(*block).wait()


def body(queries_in, keys_in, values_in, gate_rows, out_weight):
    any_space = pl.BlockSpec(memory_space=pl.ANY)
    natural = pltpu.VMEM((SEQS, T, HEADS, D), bf16)
    wide = pltpu.VMEM((HEADS * PITCH, D), f32)
    dma = pltpu.SemaphoreType.DMA
    result = pl.pallas_call(
        attention,
        out_shape=jax.ShapeDtypeStruct((SEQS, T, WIDTH), bf16),
        in_specs=[any_space] * 5,
        out_specs=any_space,
        scratch_shapes=[
            natural, natural, natural, natural,
            wide, wide, pltpu.VMEM((SEQS, HEADS * PITCH, D), f32),
            pltpu.VMEM((SEQS * HEADS, T, D), bf16),
            pltpu.VMEM((SEQS * HEADS * D, D), f32),
            pltpu.VMEM((SEQS * HEADS, D), f32),
            pltpu.VMEM((SEQS, 8, HEADS, D), f32),
            pltpu.VMEM((CHUNKS, CROWS, D), f32),
            pltpu.VMEM((CHUNKS, 2, CROWS // 4, D), f32),
            pltpu.VMEM((CHUNKS, 2, CROWS // 4, D), f32),
            pltpu.VMEM((SEQS * HEADS * D, D), bf16),
            pltpu.VMEM((SEQS, HEADS, T, D), bf16),
            pltpu.VMEM((16, 2, 2, ROWS, WIDTH), bf16),
            dma((4, SEQS, PIECES)), dma, dma((SEQS, HEADS)),
            dma((CHUNKS,)), dma((CHUNKS,)), dma((CHUNKS, 3, 2)), dma((CHUNKS, 3, 2)),
            dma((CHUNKS,)), dma((CHUNKS,)), dma((SEQS, 8)), dma((SEQS, 8)),
            dma((5, 4, 4, 2)), dma((4, 4, 2)), dma((4, 4, 2)),
        ],
        compiler_params=pltpu.CompilerParams(
            collective_id=0, has_side_effects=True, vmem_limit_bytes=63 * 1024 * 1024
        ),
        name="attention",
    )(queries_in, keys_in, values_in, gate_rows, out_weight.reshape(2, 2, ROWS, WIDTH))
    return pl.pallas_call(
        hand_over,
        out_shape=jax.ShapeDtypeStruct((SEQS, T, WIDTH), bf16),
        in_specs=[any_space],
        out_specs=any_space,
        scratch_shapes=[pltpu.VMEM((SEQS, T, WIDTH), bf16), dma((SEQS, BLOCKS)), dma((SEQS, BLOCKS))],
        compiler_params=pltpu.CompilerParams(vmem_limit_bytes=63 * 1024 * 1024),
        name="hand_over",
    )(result)


def solution(mesh):
    rows = P("outer", "span", None, None)
    return jax.shard_map(
        body, mesh=mesh, in_specs=(rows, rows, rows, rows, P("outer", None)),
        out_specs=P("outer", "span", None), check_vma=False,
    )
```
